32 devices in a mesh: ta: 4 (over y, x), sa: 8 (over z, core).
Axes of the slice: x: 2, y: 2, z: 4, core: 2. Of those that a mesh axis runs over, the one named last changes fastest.
Arguments:
- eigvecs: float32 [2, 8, 64, 3, 4096], P(None, 'ta', None, None, 'sa'), may hold values from -0.0546875 to 0.0546875
- solutions: float32 [2, 8, 3, 8, 4, 3, 4096], P(None, 'ta', None, None, None, None, 'sa'), may hold values from -15 to 15
- source_times: int32 [3], replicated, may hold values from 0 to 7, as said below
- spin_dilution: int32 [3, 8], replicated, may hold values from 0 to 3
Outputs:
- perambulator: float32 [2, 8, 6144], P(None, 'ta', 'sa')
- norms: float32 [3, 8], replicated
The draws below stay inside these ranges and needn't reach their ends.
Inputs may be any that keep to these rules, and one draw needn't show every extreme that they name: `source_times`: some source lies at slice 0 and another at slice 8 - 1.
All inputs are finite; a program needn't handle non-finite values.
Results may differ from the reference program's by a relative error of at most 0.000084.
Values sent between devices are 32-bit elements; how exact they have to be, the bound alone decides.
A program may use at most 64 MiB of HBM per device.

```python
import jax
import jax.numpy as jnp
from jax import lax

NEV = 64
NSRC = 3
COLS = 8
NT = 8
NSPACE = 4096


def times_for(key):
    base = jax.random.randint(jax.random.fold_in(key, 7), (NSRC,), 0, NT).astype(jnp.int32)
    last_pick = jax.random.randint(jax.random.fold_in(key, 8), (), 0, NSRC).astype(jnp.int32)
    step_pick = jax.random.randint(jax.random.fold_in(key, 9), (), 1, NSRC).astype(jnp.int32)
    first_pick = (last_pick + step_pick) % NSRC
    slots = jnp.arange(NSRC, dtype=jnp.int32)
    base = jnp.where(slots == last_pick, NT - 1, base)
    base = jnp.where(slots == first_pick, 0, base)
    return base.astype(jnp.int32)


def draw_source_times(key, part):
    return times_for(key)


def solution_part(key, salt):
    starts = times_for(key)
    slice_ids = jnp.arange(NT, dtype=jnp.int32)
    apart = jnp.abs(slice_ids[:, None] - starts[None, :])
    apart = jnp.minimum(apart, NT - apart).astype(jnp.float32)
    amplitude = 0.5 + 2.5 * jnp.exp(-apart * 16.0 / NT)
    shape = (NT, NSRC, COLS, 4, 3, NSPACE)
    noise_key = jax.random.fold_in(key, salt)
    noise = jnp.clip(jax.random.normal(noise_key, shape, jnp.float32), -5.0, 5.0)
    return noise * amplitude[:, :, None, None, None, None]


def draw_solutions(key, part):
    return jnp.stack([solution_part(key, 11), solution_part(key, 13)]).astype(jnp.float32)


def plant(entries, key, least, high):
    longest = entries.shape.index(max(entries.shape))
    spots = []
    for shift in (0, 1):
        where = [jax.random.randint(jax.random.fold_in(key, axis), (), 0, length) for axis, length in enumerate(entries.shape)]
        where[longest] = (where[longest] + shift) % entries.shape[longest]
        spots.append(tuple(where))
    return entries.at[spots[0]].set(least).at[spots[1]].set(high)


def level_of(stream_key, extent, shards, smallest, top_value):
    level = 1.0
    for dim, shards_of in shards:
        steps = jax.random.uniform(jax.random.fold_in(jax.random.fold_in(stream_key, 6), dim), (shards_of,), jnp.float32, smallest / len(shards), top_value / len(shards))
        level = level * jnp.repeat(jnp.exp(steps), extent[dim] // shards_of).reshape((-1,) + (1,) * (len(extent) - 1 - dim))
    return level


def centred(own_key, shape, width, bound, pieces=(), held_as=jnp.bfloat16):
    loudness = level_of(own_key, shape, pieces, -0.22, 0.18) if pieces else 1.0
    array = jax.random.normal(own_key, shape, jnp.float32) * width * loudness
    return jnp.minimum(jnp.maximum(array, -bound), bound).astype(held_as)


def setup_inputs(seed: int = 0) -> dict:
    seeds = jax.random.split(jax.random.key(seed), 5)
    eigvecs = centred(seeds[0], (2, NT, NEV, 3, NSPACE), (3 * NSPACE) ** -0.5, 0.0546875, ((1, 4), (4, 8)), jnp.float32)
    solutions = draw_solutions(jax.random.fold_in(seeds[4], 71), 0)
    source_times = draw_source_times(jax.random.fold_in(seeds[4], 71), 0)
    spin_dilution = plant(jax.random.randint(seeds[3], (NSRC, COLS), 0, 4), jax.random.fold_in(seeds[3], 1), 0, 3).astype(jnp.int32)
    return dict(eigvecs=eigvecs, solutions=solutions, source_times=source_times, spin_dilution=spin_dilution)


def slice_tile(inputs):
    eig_real, eig_imag, sol_real, sol_imag = inputs
    precise = lax.Precision.HIGHEST
    real_part = jnp.dot(eig_real, sol_real.T, precision=precise, preferred_element_type=jnp.float32) + jnp.dot(eig_imag, sol_imag.T, precision=precise, preferred_element_type=jnp.float32)
    imag_part = jnp.dot(eig_real, sol_imag.T, precision=precise, preferred_element_type=jnp.float32) - jnp.dot(eig_imag, sol_real.T, precision=precise, preferred_element_type=jnp.float32)
    return jnp.stack([real_part, imag_part])


def reference(eigvecs, solutions, source_times, spin_dilution):
    slice_count = eigvecs.shape[1]
    eig_count = eigvecs.shape[2]
    site_count = eigvecs.shape[4]
    src_count = spin_dilution.shape[0]
    col_count = spin_dilution.shape[1]
    columns = src_count * col_count * 4
    inner_len = 3 * site_count
    eigen_rows = eigvecs.reshape(2, slice_count, eig_count, inner_len)
    solution_rows = solutions.reshape(2, slice_count, columns, inner_len)
    tiles = lax.map(slice_tile, (eigen_rows[0], eigen_rows[1], solution_rows[0], solution_rows[1]))
    tiles = jnp.transpose(tiles, (1, 0, 2, 3))
    slice_times = jnp.arange(slice_count, dtype=jnp.int32)
    boundary = jnp.where(slice_times[:, None] < source_times[None, :], -1.0, 1.0).astype(jnp.float32)
    chirality = jnp.where(spin_dilution < 2, 1.0, -1.0).astype(jnp.float32)
    signs = jnp.broadcast_to((boundary[:, :, None] * chirality[None])[:, :, :, None], (slice_count, src_count, col_count, 4)).reshape(slice_count, columns)
    perambulator = (tiles * signs[None, :, None, :]).reshape(2, slice_count, eig_count * columns)
    norms = jnp.sum(solutions * solutions, axis=(0, 1, 4, 5, 6)) / (12.0 * slice_count * site_count)
    return perambulator, norms
```

```python
import functools
import math

import jax
import jax.numpy as jnp
from jax import lax
from jax.experimental import pallas as pl
from jax.experimental.pallas import tpu as pltpu
from jax.sharding import PartitionSpec as P

LANES = 128
DIRECT = 64
NT_DIMS = (((1,), (1,)), ((), ()))


def split_two(x):
    high = x.astype(jnp.bfloat16)
    low = (x - high.astype(jnp.float32)).astype(jnp.bfloat16)
    return high, low


def kernel(
    dims,
    eig_hbm, sol_hbm, times_hbm, spin_hbm,
    out_ref, norm_ref,
    eig_buf, sol_buf, left, right_hi, right_lo, tile_buf, flat_buf,
    send_buf, recv_buf, norm_send, norm_recv,
    times_ref, spin_ref, small_sem, own_sem,
    eig_sem, sol_sem, out_sems, in_sems, norm_out_sems, norm_in_sems,
):
    n_ta, n_sa, parts, slices, eigs, colors, sites, srcs, cols, spins, width = dims
    columns = srcs * cols * spins
    rows_own = width // LANES
    blocks = sites // LANES
    my_ta, my_sa = lax.axis_index("ta"), lax.axis_index("sa")

    barrier = pltpu.get_barrier_semaphore()
    one_phase = n_ta * n_sa <= DIRECT
    every = [(a, b) for a in range(n_ta) for b in range(n_sa) if a or b]
    over_sa = [(0, b) for b in range(1, n_sa)]
    over_ta = [(a, 0) for a in range(1, n_ta)]
    first, second = (every, []) if one_phase else (over_sa, over_ta)

    def device(offs):
        return {
            "ta": lax.rem(my_ta + offs[0], n_ta),
            "sa": lax.rem(my_sa + offs[1], n_sa),
        }

    for offs in first + second:
        pl.semaphore_signal(barrier, inc=1, device_id=device(offs))

    small_copies = [
        pltpu.make_async_copy(times_hbm, times_ref, small_sem.at[0]),
        pltpu.make_async_copy(spin_hbm, spin_ref, small_sem.at[1]),
    ]
    for copy in small_copies:
        copy.start()
    sol_copies, eig_copies = {}, {}
    for t in range(slices):
        for c in range(colors):
            for j in range(blocks):
                at = (t * colors + c) * blocks + j
                copy = pltpu.make_async_copy(
                    sol_hbm.at[:, t, :, c, :, pl.ds(j * LANES, LANES)],
                    sol_buf.at[at].reshape(parts, srcs * cols, spins, LANES),
                    sol_sem.at[at],
                )
                copy.start()
                sol_copies[t, c, j] = copy
            copy = pltpu.make_async_copy(
                eig_hbm.at[:, t, c], eig_buf.at[t * colors + c], eig_sem.at[t * colors + c]
            )
            copy.start()
            eig_copies[t, c] = copy

    for copy in small_copies:
        copy.wait()
    lane = lax.broadcasted_iota(jnp.int32, (8, LANES), 1)
    chir = jnp.ones((8, LANES), jnp.float32)
    group = lane // spins
    for s in range(srcs):
        for k in range(cols):
            value = jnp.where(spin_ref[s, k] < 2, 1.0, -1.0)
            chir = jnp.where(group == s * cols + k, value, chir)
    source = lane // (spins * cols)
    signs = []
    for t in range(slices):
        now = my_ta * slices + t
        sign = chir
        for s in range(srcs):
            value = jnp.where(now < times_ref[s], -1.0, 1.0)
            sign = jnp.where(source == s, chir * value, sign)
        signs.append(sign[:1])

    period = math.lcm(columns, LANES)
    rows_in, rows_out = period // columns, period // LANES
    groups = eigs // rows_in
    lane_g = lax.broadcasted_iota(jnp.int32, (groups, LANES), 1)
    copies, owns = {}, []
    rows = parts * rows_own
    sub = math.gcd(rows, 4)

    def make_tiles(t):
        both = lax.dot_general(
            left[t], right_hi[t], NT_DIMS, preferred_element_type=jnp.float32
        )
        cross = lax.dot_general(
            left[t, : parts * eigs, :], right_lo[t], NT_DIMS,
            preferred_element_type=jnp.float32,
        )
        g = both[: parts * eigs] + both[parts * eigs :] + cross
        tiles = (
            g[:eigs, :LANES] + g[eigs:, LANES:],
            g[:eigs, LANES:] - g[eigs:, :LANES],
        )
        for p in range(parts):
            tile_buf[t, p] = tiles[p] * signs[t]
            taken = [tile_buf[t, p, pl.ds(i, groups, stride=rows_in), :] for i in range(rows_in)]
            for o in range(rows_out):
                value, filled = None, 0
                while filled < LANES:
                    i, skip = divmod(o * LANES + filled, columns)
                    size = min(columns - skip, LANES - filled)
                    shift = (filled - skip) % LANES
                    piece = pltpu.roll(taken[i], shift, 1) if shift else taken[i]
                    value = piece if value is None else jnp.where(lane_g < filled, value, piece)
                    filled += size
                flat_buf[t, p, pl.ds(o, groups, stride=rows_out), :] = value
            for d in range(n_sa):
                send_buf[t, pl.ds(d * rows + p * rows_own, rows_own), :] = flat_buf[
                    t, p, pl.ds(d * rows_own, rows_own), :
                ]

    def send_tiles(t):
        sent = send_buf.at[t].reshape(n_sa, rows // sub, sub, LANES)
        landed = recv_buf.at[t].reshape(n_sa, rows // sub, sub, LANES)
        for off in range(1, n_sa):
            peer = lax.rem(my_sa + off, n_sa)
            copy = pltpu.make_async_remote_copy(
                src_ref=sent.at[peer],
                dst_ref=landed.at[off - 1],
                send_sem=out_sems.at[t, off - 1],
                recv_sem=in_sems.at[t, off - 1],
                device_id={"sa": peer},
            )
            copy.start()
            copies[t, off] = copy
        own = pltpu.make_async_copy(sent.at[my_sa], landed.at[n_sa - 1], own_sem.at[t])
        own.start()
        owns.append(own)

    inner = colors * sites
    pad = LANES - columns
    if pad:
        for t in range(slices):
            for p in range(parts):
                spare = pl.ds(p * LANES + columns, pad)
                right_hi[t, spare, :] = jnp.zeros((pad, inner), jnp.bfloat16)
                right_lo[t, spare, :] = jnp.zeros((pad, inner), jnp.bfloat16)
    squares = jnp.zeros((columns, LANES), jnp.float32)
    for t in range(slices):
        for c in range(colors):
            for j in range(blocks):
                sol_copies[t, c, j].wait()
                lanes = pl.ds(c * sites + j * LANES, LANES)
                for p in range(parts):
                    x = sol_buf[(t * colors + c) * blocks + j, p]
                    squares = squares + x * x
                    high, low = split_two(x)
                    right_hi[t, pl.ds(p * LANES, columns), lanes] = high
                    right_lo[t, pl.ds(p * LANES, columns), lanes] = low
            eig_copies[t, c].wait()
            lanes = pl.ds(c * sites, sites)
            for p in range(parts):
                high, low = split_two(eig_buf[t * colors + c, p])
                left[t, pl.ds(p * eigs, eigs), lanes] = high
                left[t, pl.ds((parts + p) * eigs, eigs), lanes] = low
        if t < slices - 1:
            make_tiles(t)

    pl.semaphore_wait(barrier, len(first + second))

    precise = lax.Precision.HIGHEST
    lane_sums = lax.dot_general(
        jnp.ones((8, LANES), jnp.float32), squares, NT_DIMS,
        precision=precise, preferred_element_type=jnp.float32,
    )
    wanted = lax.broadcasted_iota(jnp.int32, (LANES, columns), 0)
    given = lax.broadcasted_iota(jnp.int32, (LANES, columns), 1) // spins
    picks = jnp.where(wanted == given, 1.0, 0.0).astype(jnp.float32)
    own_norm = lax.dot_general(
        lane_sums, picks, NT_DIMS, precision=precise, preferred_element_type=jnp.float32
    )[:1]
    norm_copies = []

    def send_norm(phase, base, peers):
        for at, offs in enumerate(peers):
            copy = pltpu.make_async_remote_copy(
                src_ref=norm_send.at[phase],
                dst_ref=norm_recv.at[base + at],
                send_sem=norm_out_sems.at[base + at],
                recv_sem=norm_in_sems.at[base + at],
                device_id=device(offs),
            )
            copy.start()
            norm_copies.append(copy)

    norm_send[0] = own_norm
    send_norm(0, 0, first)

    for t in range(slices):
        if t == slices - 1:
            make_tiles(t)
        send_tiles(t)

    if second:
        for at, copy in enumerate(norm_copies):
            copy.wait_recv()
            own_norm = own_norm + norm_recv[at]
        norm_send[1] = own_norm
        send_norm(1, len(first), second)

    for t in range(slices):
        owns[t].wait()
        total = recv_buf[t, pl.ds((n_sa - 1) * rows, rows), :]
        for off in range(1, n_sa):
            copies[t, off].wait_recv()
            total = total + recv_buf[t, pl.ds((off - 1) * rows, rows), :]
        for p in range(parts):
            for r in range(rows_own):
                row = p * rows_own + r
                out_ref[p, pl.ds(t, 1), pl.ds(r * LANES, LANES)] = total[row : row + 1]
    landed_from = len(first) if second else 0
    for copy in norm_copies[landed_from:]:
        copy.wait_recv()
    own_norm = own_norm + jnp.sum(norm_recv[landed_from:], axis=0)
    cells = 1.0 * spins * colors * slices * n_ta * sites * n_sa
    own_norm = own_norm / cells
    for s in range(srcs):
        norm_ref[pl.ds(s, 1), :] = own_norm[:, s * cols : (s + 1) * cols]
    for copy in norm_copies:
        copy.wait_send()
    for copy in copies.values():
        copy.wait_send()


def hand_over(tiles_ref, norms_ref, out_hbm, norm_hbm, sems):
    copies = [
        pltpu.make_async_copy(tiles_ref, out_hbm, sems.at[0]),
        pltpu.make_async_copy(norms_ref, norm_hbm, sems.at[1]),
    ]
    for copy in copies:
        copy.start()
    for copy in copies:
        copy.wait()


def on_device(eigvecs, solutions, source_times, spin_dilution):
    n_ta, n_sa = lax.axis_size("ta"), lax.axis_size("sa")
    parts, slices, eigs, colors, sites = eigvecs.shape
    _, _, srcs, cols, spins, _, _ = solutions.shape
    columns = srcs * cols * spins
    width = eigs * columns // n_sa
    eig_view = jnp.transpose(eigvecs, (0, 1, 3, 2, 4))
    sol_view = jnp.transpose(solutions, (0, 1, 2, 3, 5, 4, 6)).reshape(
        parts, slices, srcs * cols, colors, spins, sites
    )
    dims = (n_ta, n_sa, parts, slices, eigs, colors, sites, srcs, cols, spins, width)
    blocks = sites // LANES
    inner = colors * sites
    rows = parts * (width // LANES)
    norm_peers = n_ta * n_sa - 1 if n_ta * n_sa <= DIRECT else n_ta + n_sa - 2
    f32, bf16 = jnp.float32, jnp.bfloat16
    dma = pltpu.SemaphoreType.DMA
    tiles, norms = pl.pallas_call(
        functools.partial(kernel, dims),
        out_shape=(
            pltpu.VMEM((parts, slices, width), f32),
            pltpu.VMEM((srcs, cols), f32),
        ),
        in_specs=[
            pl.BlockSpec(memory_space=pltpu.HBM),
            pl.BlockSpec(memory_space=pltpu.HBM),
            pl.BlockSpec(memory_space=pltpu.HBM),
            pl.BlockSpec(memory_space=pltpu.HBM),
        ],
        out_specs=(
            pl.BlockSpec(memory_space=pltpu.VMEM),
            pl.BlockSpec(memory_space=pltpu.VMEM),
        ),
        scratch_shapes=[
            pltpu.VMEM((slices * colors, parts, eigs, sites), f32),
            pltpu.VMEM((slices * colors * blocks, parts, columns, LANES), f32),
            pltpu.VMEM((slices, 2 * parts * eigs, inner), bf16),
            pltpu.VMEM((slices, parts * LANES, inner), bf16),
            pltpu.VMEM((slices, parts * LANES, inner), bf16),
            pltpu.VMEM((slices, parts, eigs, LANES), f32),
            pltpu.VMEM((slices, parts, eigs * columns // LANES, LANES), f32),
            pltpu.VMEM((slices, n_sa * rows, LANES), f32),
            pltpu.VMEM((slices, n_sa * rows, LANES), f32),
            pltpu.VMEM((2, 1, LANES), f32),
            pltpu.VMEM((norm_peers, 1, LANES), f32),
            pltpu.SMEM((srcs,), jnp.int32),
            pltpu.SMEM((srcs, cols), jnp.int32),
            dma((2,)),
            dma((slices,)),
            dma((slices * colors,)),
            dma((slices * colors * blocks,)),
            dma((slices, n_sa - 1)),
            dma((slices, n_sa - 1)),
            dma((norm_peers,)),
            dma((norm_peers,)),
        ],
        compiler_params=pltpu.CompilerParams(collective_id=0, has_side_effects=True, vmem_limit_bytes=66 * 10**6),
    )(eig_view, sol_view, source_times, spin_dilution)
    return pl.pallas_call(
        hand_over,
        out_shape=(
            jax.ShapeDtypeStruct(tiles.shape, f32),
            jax.ShapeDtypeStruct(norms.shape, f32),
        ),
        in_specs=[pl.BlockSpec(memory_space=pltpu.VMEM)] * 2,
        out_specs=[pl.BlockSpec(memory_space=pltpu.HBM)] * 2,
        scratch_shapes=[dma((2,))],
        compiler_params=pltpu.CompilerParams(vmem_limit_bytes=2**20),
    )(tiles, norms)


def solution(mesh):
    return jax.shard_map(
        on_device,
        mesh=mesh,
        in_specs=(
            P(None, "ta", None, None, "sa"),
            P(None, "ta", None, None, None, None, "sa"),
            P(),
            P(),
        ),
        out_specs=(P(None, "ta", "sa"), P()),
        check_vma=False,
    )
```

```python
import functools
import math

import jax
import jax.numpy as jnp
from jax import lax
from jax.experimental import pallas as pl
from jax.experimental.pallas import tpu as pltpu
from jax.sharding import PartitionSpec as P

LANES = 128
SUBLANES = 8
DIRECT = 64
NT_DIMS = (((1,), (1,)), ((), ()))


def split_two(x):
    high = x.astype(jnp.bfloat16)
    low = (x - high.astype(jnp.float32)).astype(jnp.bfloat16)
    return high, low


def others(count, me):
    for k in range(count - 1):
        past = (me <= k).astype(jnp.int32)
        yield k + past, me - 1 + past


def wait_for(ref, sem):
    pltpu.make_async_copy(ref, ref, sem).wait()


def whole_rows(eigs, n_sa):
    return eigs % (SUBLANES * n_sa) == 0


def kernel(
    dims,
    eig_hbm, sol_hbm, times_hbm, spin_hbm,
    out_ref, norm_ref,
    eig_buf, sol_buf, left, right_hi, right_lo, tile_buf, flat_buf,
    send_buf, recv_buf, norm_send, norm_recv,
    times_ref, spin_ref, small_sem,
    eig_sem, sol_sem, out_sems, in_sems, norm_out_sems, norm_in_sems,
):
    n_ta, n_sa, parts, slices, eigs, colors, sites, srcs, cols, spins, width = dims
    columns = srcs * cols * spins
    rows_own = width // LANES
    blocks = sites // LANES
    by_row = whole_rows(eigs, n_sa)
    piece = eigs // n_sa if by_row else rows_own
    rows = parts * piece
    sub = math.gcd(rows, SUBLANES)
    my_ta, my_sa = lax.axis_index("ta"), lax.axis_index("sa")
    barrier = pltpu.get_barrier_semaphore()

    def flat_device(at):
        return {"ta": lax.div(at, n_sa), "sa": lax.rem(at, n_sa)}

    if n_ta * n_sa <= DIRECT:
        groups = [(n_ta * n_sa, my_ta * n_sa + my_sa, flat_device)]
    else:
        groups = [
            (n_sa, my_sa, lambda at: {"sa": at}),
            (n_ta, my_ta, lambda at: {"ta": at}),
        ]
    chunks = [(t, c) for t in range(slices) for c in range(colors)]

    for t, c in chunks:
        for j in range(blocks):
            at = (t * colors + c) * blocks + j
            pltpu.make_async_copy(
                sol_hbm.at[:, t, :, c, :, pl.ds(j * LANES, LANES)],
                sol_buf.at[at].reshape(parts, srcs * cols, spins, LANES),
                sol_sem.at[t * colors + c],
            ).start()
    for count, me, device in groups:
        for peer, _ in others(count, me):
            pl.semaphore_signal(barrier, inc=1, device_id=device(peer))
    for t, c in chunks:
        pltpu.make_async_copy(
            eig_hbm.at[:, t, c], eig_buf.at[t * colors + c], eig_sem.at[t * colors + c]
        ).start()
    small_copies = [
        pltpu.make_async_copy(times_hbm, times_ref, small_sem.at[0]),
        pltpu.make_async_copy(spin_hbm, spin_ref, small_sem.at[1]),
    ]
    for copy in small_copies:
        copy.start()

    inner = colors * sites
    pad = LANES - columns
    if pad:
        for t in range(slices):
            for p in range(parts):
                spare = pl.ds(p * LANES + columns, pad)
                right_hi[t, spare, :] = jnp.zeros((pad, inner), jnp.bfloat16)
                right_lo[t, spare, :] = jnp.zeros((pad, inner), jnp.bfloat16)

    def sol_blocks(t, c):
        for j in range(blocks):
            lanes = pl.ds(c * sites + j * LANES, LANES)
            for p in range(parts):
                yield p, lanes, sol_buf[(t * colors + c) * blocks + j, p]

    def split_sol(t, c):
        for p, lanes, x in sol_blocks(t, c):
            high, low = split_two(x)
            right_hi[t, pl.ds(p * LANES, columns), lanes] = high
            right_lo[t, pl.ds(p * LANES, columns), lanes] = low

    def split_eig(t, c):
        lanes = pl.ds(c * sites, sites)
        for p in range(parts):
            high, low = split_two(eig_buf[t * colors + c, p])
            left[t, pl.ds(p * eigs, eigs), lanes] = high
            left[t, pl.ds((parts + p) * eigs, eigs), lanes] = low

    squares = jnp.zeros((columns, LANES), jnp.float32)
    for t, c in chunks:
        at = t * colors + c
        wait_for(sol_buf.at[pl.ds(at * blocks, blocks)], sol_sem.at[at])
        for _, _, x in sol_blocks(t, c):
            squares = squares + x * x
        if (t, c) != chunks[-1]:
            split_sol(t, c)

    cells = 1.0 * spins * colors * slices * n_ta * sites * n_sa
    sums = jnp.sum(squares, axis=1, keepdims=True) * (1.0 / cells)
    lane = lax.broadcasted_iota(jnp.int32, (columns, LANES), 1)
    group = lax.broadcasted_iota(jnp.int32, (columns, LANES), 0) // spins
    own_norm = jnp.sum(jnp.where(lane == group, sums, 0.0), axis=0, keepdims=True)
    bases = [0, groups[0][0] - 1]

    def send_norm(phase):
        count, me, device = groups[phase]
        for peer, slot in others(count, me):
            pltpu.make_async_remote_copy(
                src_ref=norm_send.at[phase],
                dst_ref=norm_recv.at[bases[phase] + slot],
                send_sem=norm_out_sems.at[phase],
                recv_sem=norm_in_sems.at[phase],
                device_id=device(peer),
            ).start()

    def norm_rows(phase):
        return norm_recv.at[pl.ds(bases[phase], groups[phase][0] - 1)]

    norm_send[0] = own_norm
    pl.semaphore_wait(barrier, sum(count - 1 for count, _, _ in groups))
    send_norm(0)
    split_sol(*chunks[-1])

    def make_signs():
        for copy in small_copies:
            copy.wait()
        lane = lax.broadcasted_iota(jnp.int32, (SUBLANES, LANES), 1)
        chir = jnp.ones((SUBLANES, LANES), jnp.float32)
        for s in range(srcs):
            for k in range(cols):
                value = jnp.where(spin_ref[s, k] < 2, 1.0, -1.0)
                chir = jnp.where(lane // spins == s * cols + k, value, chir)
        signs = []
        for t in range(slices):
            now = my_ta * slices + t
            sign = chir
            for s in range(srcs):
                value = jnp.where(now < times_ref[s], -1.0, 1.0)
                sign = jnp.where(lane // (spins * cols) == s, chir * value, sign)
            signs.append(sign)
        return signs

    def partial(t, c):
        lanes = pl.ds(c * sites, sites)
        both = lax.dot_general(
            left[t, :, lanes], right_hi[t, :, lanes], NT_DIMS,
            preferred_element_type=jnp.float32,
        )
        cross = lax.dot_general(
            left[t, : parts * eigs, lanes], right_lo[t, :, lanes], NT_DIMS,
            preferred_element_type=jnp.float32,
        )
        return both[: parts * eigs] + both[parts * eigs :] + cross

    def flatten(t, p, tile):
        period = math.lcm(columns, LANES)
        rows_in, rows_out = period // columns, period // LANES
        count = eigs // rows_in
        lane = lax.broadcasted_iota(jnp.int32, (count, LANES), 1)
        tile_buf[t, p] = tile
        taken = [tile_buf[t, p, pl.ds(i, count, stride=rows_in), :] for i in range(rows_in)]
        for o in range(rows_out):
            value, filled = None, 0
            while filled < LANES:
                i, skip = divmod(o * LANES + filled, columns)
                size = min(columns - skip, LANES - filled)
                shift = (filled - skip) % LANES
                part = pltpu.roll(taken[i], shift, 1) if shift else taken[i]
                value = part if value is None else jnp.where(lane < filled, value, part)
                filled += size
            flat_buf[t, p, pl.ds(o, count, stride=rows_out), :] = value

    def store_tiles(t, g):
        tiles = (
            g[:eigs, :LANES] + g[eigs:, LANES:],
            g[:eigs, LANES:] - g[eigs:, :LANES],
        )
        for p in range(parts):
            if not by_row:
                flatten(t, p, tiles[p] * signs[t][:1])
            for d in range(n_sa):
                mine = slice(d * piece, (d + 1) * piece)
                send_buf[t, pl.ds(d * rows + p * piece, piece), :] = (
                    tiles[p][mine] if by_row else flat_buf[t, p, mine, :]
                )

    def send_tiles(t):
        sent = send_buf.at[t].reshape(n_sa, rows // sub, sub, LANES)
        landed = recv_buf.at[t].reshape(n_sa - 1, rows // sub, sub, LANES)
        for peer, slot in others(n_sa, my_sa):
            pltpu.make_async_remote_copy(
                src_ref=sent.at[peer],
                dst_ref=landed.at[slot],
                send_sem=out_sems.at[t],
                recv_sem=in_sems.at[t],
                device_id={"sa": peer},
            ).start()

    def step(t, c, g):
        g = partial(t, c) if c == 0 else g + partial(t, c)
        if c == colors - 1:
            store_tiles(t, g)
            send_tiles(t)
        return g

    signs = None if by_row else make_signs()
    g, last = None, None
    for t, c in chunks:
        at = t * colors + c
        wait_for(eig_buf.at[at], eig_sem.at[at])
        split_eig(t, c)
        if last is not None:
            g = step(*last, g)
        last = t, c
    step(*last, g)

    if len(groups) > 1:
        wait_for(norm_rows(0), norm_in_sems.at[0])
        own_norm = own_norm + jnp.sum(norm_rows(0)[...], axis=0)
        norm_send[1] = own_norm
        send_norm(1)

    if by_row:
        signs = make_signs()
    lane_own = lax.broadcasted_iota(jnp.int32, (1, LANES), 1)
    for t in range(slices):
        wait_for(recv_buf.at[t], in_sems.at[t])
        total = send_buf[t, pl.ds(my_sa * rows, rows), :]
        for slot in range(n_sa - 1):
            total = total + recv_buf[t, pl.ds(slot * rows, rows), :]
        for p in range(parts):
            own = total[p * piece : (p + 1) * piece]
            if by_row:
                own = own.reshape(piece // SUBLANES, SUBLANES, LANES) * signs[t]
                own = own.reshape(piece, LANES)
                turned = {}
            for r in range(rows_own):
                if by_row:
                    value, filled = None, 0
                    while filled < LANES:
                        i, skip = divmod(r * LANES + filled, columns)
                        shift = (filled - skip) % LANES
                        if shift not in turned:
                            turned[shift] = pltpu.roll(own, shift, 1) if shift else own
                        part = turned[shift][i : i + 1]
                        value = part if value is None else jnp.where(lane_own < filled, value, part)
                        filled += min(columns - skip, LANES - filled)
                else:
                    value = own[r : r + 1]
                out_ref[p, pl.ds(t, 1), pl.ds(r * LANES, LANES)] = value
        wait_for(recv_buf.at[t], out_sems.at[t])
    for phase in range(len(groups)):
        wait_for(norm_rows(phase), norm_out_sems.at[phase])
    final = len(groups) - 1
    wait_for(norm_rows(final), norm_in_sems.at[final])
    own_norm = own_norm + jnp.sum(norm_rows(final)[...], axis=0)
    for s in range(srcs):
        row = pltpu.roll(own_norm, LANES - s * cols, 1) if s else own_norm
        norm_ref[pl.ds(s, 1), :] = row[:, :cols]


def hand_over(tiles_ref, norms_ref, out_hbm, norm_hbm, sems):
    copies = [
        pltpu.make_async_copy(tiles_ref, out_hbm, sems.at[0]),
        pltpu.make_async_copy(norms_ref, norm_hbm, sems.at[1]),
    ]
    for copy in copies:
        copy.start()
    for copy in copies:
        copy.wait()


def on_device(eigvecs, solutions, source_times, spin_dilution):
    n_ta, n_sa = lax.axis_size("ta"), lax.axis_size("sa")
    parts, slices, eigs, colors, sites = eigvecs.shape
    _, _, srcs, cols, spins, _, _ = solutions.shape
    columns = srcs * cols * spins
    width = eigs * columns // n_sa
    eig_view = jnp.transpose(eigvecs, (0, 1, 3, 2, 4))
    sol_view = jnp.transpose(solutions, (0, 1, 2, 3, 5, 4, 6)).reshape(
        parts, slices, srcs * cols, colors, spins, sites
    )
    dims = (n_ta, n_sa, parts, slices, eigs, colors, sites, srcs, cols, spins, width)
    blocks = sites // LANES
    inner = colors * sites
    rows = parts * (eigs // n_sa if whole_rows(eigs, n_sa) else width // LANES)
    norm_peers = n_ta * n_sa - 1 if n_ta * n_sa <= DIRECT else n_ta + n_sa - 2
    f32, bf16 = jnp.float32, jnp.bfloat16
    dma = pltpu.SemaphoreType.DMA
    tiles, norms = pl.pallas_call(
        functools.partial(kernel, dims),
        out_shape=(
            pltpu.VMEM((parts, slices, width), f32),
            pltpu.VMEM((srcs, cols), f32),
        ),
        in_specs=[
            pl.BlockSpec(memory_space=pltpu.HBM),
            pl.BlockSpec(memory_space=pltpu.HBM),
            pl.BlockSpec(memory_space=pltpu.HBM),
            pl.BlockSpec(memory_space=pltpu.HBM),
        ],
        out_specs=(
            pl.BlockSpec(memory_space=pltpu.VMEM),
            pl.BlockSpec(memory_space=pltpu.VMEM),
        ),
        scratch_shapes=[
            pltpu.VMEM((slices * colors, parts, eigs, sites), f32),
            pltpu.VMEM((slices * colors * blocks, parts, columns, LANES), f32),
            pltpu.VMEM((slices, 2 * parts * eigs, inner), bf16),
            pltpu.VMEM((slices, parts * LANES, inner), bf16),
            pltpu.VMEM((slices, parts * LANES, inner), bf16),
            pltpu.VMEM((slices, parts, eigs, LANES), f32),
            pltpu.VMEM((slices, parts, eigs * columns // LANES, LANES), f32),
            pltpu.VMEM((slices, n_sa * rows, LANES), f32),
            pltpu.VMEM((slices, (n_sa - 1) * rows, LANES), f32),
            pltpu.VMEM((2, 1, LANES), f32),
            pltpu.VMEM((norm_peers, 1, LANES), f32),
            pltpu.SMEM((srcs,), jnp.int32),
            pltpu.SMEM((srcs, cols), jnp.int32),
            dma((2,)),
            dma((slices * colors,)),
            dma((slices * colors,)),
            dma((slices,)),
            dma((slices,)),
            dma((2,)),
            dma((2,)),
        ],
        compiler_params=pltpu.CompilerParams(
            collective_id=0, has_side_effects=True, vmem_limit_bytes=66 * 10**6
        ),
    )(eig_view, sol_view, source_times, spin_dilution)
    return pl.pallas_call(
        hand_over,
        out_shape=(
            jax.ShapeDtypeStruct(tiles.shape, f32),
            jax.ShapeDtypeStruct(norms.shape, f32),
        ),
        in_specs=[pl.BlockSpec(memory_space=pltpu.VMEM)] * 2,
        out_specs=[pl.BlockSpec(memory_space=pltpu.HBM)] * 2,
        scratch_shapes=[dma((2,))],
        compiler_params=pltpu.CompilerParams(vmem_limit_bytes=2**20),
    )(tiles, norms)


def solution(mesh):
    return jax.shard_map(
        on_device,
        mesh=mesh,
        in_specs=(
            P(None, "ta", None, None, "sa"),
            P(None, "ta", None, None, None, None, "sa"),
            P(),
            P(),
        ),
        out_specs=(P(None, "ta", "sa"), P()),
        check_vma=False,
    )
```

```python
import functools
import math

import jax
import jax.numpy as jnp
from jax import lax
from jax.experimental import pallas as pl
from jax.experimental.pallas import tpu as pltpu
from jax.sharding import PartitionSpec as P

LANES = 128
SUBLANES = 8
DIRECT = 64
NT_DIMS = (((1,), (1,)), ((), ()))


def split_two(x):
    high = x.astype(jnp.bfloat16)
    low = (x - high.astype(jnp.float32)).astype(jnp.bfloat16)
    return high, low


def others(count, me):
    for k in range(count - 1):
        past = (me <= k).astype(jnp.int32)
        yield k + past, me - 1 + past


def wait_for(ref, sem):
    pltpu.make_async_copy(ref, ref, sem).wait()


def can_pack(parts, slices, eigs, columns, n_sa):
    return (
        parts == slices == 2 and parts * eigs == LANES
        and 4 * columns == 3 * LANES and eigs % (SUBLANES * n_sa) == 0
    )


def kernel(
    dims,
    eig_hbm, sol_hbm, times_hbm, spin_hbm,
    out_ref, norm_ref,
    eig_buf, sol_buf, eig_split, sol_split, tile_buf, flat_buf,
    send_buf, recv_buf, norm_send, norm_recv,
    times_ref, spin_ref, small_sem,
    eig_sem, sol_sem, out_sem, in_sem, norm_out_sems, norm_in_sems,
):
    n_ta, n_sa, parts, slices, eigs, colors, sites, srcs, cols, spins, width = dims
    columns = srcs * cols * spins
    rows_own = width // LANES
    blocks = sites // LANES
    packed = can_pack(parts, slices, eigs, columns, n_sa)
    pad = LANES - columns
    piece = eigs // n_sa if packed else rows_own
    rows = parts * rows_own
    share = 3 * piece if packed else slices * rows
    sub = math.gcd(share, SUBLANES)
    my_ta, my_sa = lax.axis_index("ta"), lax.axis_index("sa")
    barrier = pltpu.get_barrier_semaphore()

    def flat_device(at):
        return {"ta": lax.div(at, n_sa), "sa": lax.rem(at, n_sa)}

    if n_ta * n_sa <= DIRECT:
        groups = [(n_ta * n_sa, my_ta * n_sa + my_sa, flat_device)]
    else:
        groups = [
            (n_sa, my_sa, lambda at: {"sa": at}),
            (n_ta, my_ta, lambda at: {"ta": at}),
        ]
    chunks = [(t, c) for t in range(slices) for c in range(colors)]

    for t, c in chunks:
        for j in range(blocks):
            at = (t * colors + c) * blocks + j
            pltpu.make_async_copy(
                sol_hbm.at[:, t, :, c, :, pl.ds(j * LANES, LANES)],
                sol_buf.at[at].reshape(parts, srcs * cols, spins, LANES),
                sol_sem.at[t * colors + c],
            ).start()
    for count, me, device in groups:
        for peer, _ in others(count, me):
            pl.semaphore_signal(barrier, inc=1, device_id=device(peer))
    for c in range(colors):
        for t in range(slices):
            pltpu.make_async_copy(
                eig_hbm.at[:, t, c], eig_buf.at[c, t], eig_sem.at[c]
            ).start()
    small_copies = [
        pltpu.make_async_copy(times_hbm, times_ref, small_sem.at[0]),
        pltpu.make_async_copy(spin_hbm, spin_ref, small_sem.at[1]),
    ]
    for copy in small_copies:
        copy.start()

    def sol_blocks(t, c):
        for j in range(blocks):
            lanes = pl.ds(c * sites + j * LANES, LANES)
            for p in range(parts):
                yield p, lanes, sol_buf[(t * colors + c) * blocks + j, p]

    def split_sol(t, c):
        for p, lanes, x in sol_blocks(t, c):
            high, low = split_two(x)
            sol_split[t, pl.ds(p * columns, columns), lanes] = high
            sol_split[t, pl.ds((parts + p) * columns, columns), lanes] = low

    def split_eig(t, c):
        lanes = pl.ds(c * sites, sites)
        for p in range(parts):
            high, low = split_two(eig_buf[c, t, p])
            eig_split[t, pl.ds(p * eigs, eigs), lanes] = high
            eig_split[t, pl.ds((parts + p) * eigs, eigs), lanes] = low

    squares = jnp.zeros((columns, LANES), jnp.float32)
    for t, c in chunks:
        at = t * colors + c
        wait_for(sol_buf.at[pl.ds(at * blocks, blocks)], sol_sem.at[at])
        for _, _, x in sol_blocks(t, c):
            squares = squares + x * x
        if (t, c) != chunks[-1]:
            split_sol(t, c)

    cells = 1.0 * spins * colors * slices * n_ta * sites * n_sa
    sums = jnp.sum(squares, axis=1, keepdims=True) * (1.0 / cells)
    lane = lax.broadcasted_iota(jnp.int32, (columns, LANES), 1)
    group = lax.broadcasted_iota(jnp.int32, (columns, LANES), 0) // spins
    own_norm = jnp.sum(jnp.where(lane == group, sums, 0.0), axis=0, keepdims=True)
    bases = [0, groups[0][0] - 1]

    def send_norm(phase):
        count, me, device = groups[phase]
        for peer, slot in others(count, me):
            pltpu.make_async_remote_copy(
                src_ref=norm_send.at[phase],
                dst_ref=norm_recv.at[bases[phase] + slot],
                send_sem=norm_out_sems.at[phase],
                recv_sem=norm_in_sems.at[phase],
                device_id=device(peer),
            ).start()

    def norm_rows(phase):
        return norm_recv.at[pl.ds(bases[phase], groups[phase][0] - 1)]

    norm_send[0] = own_norm
    last_chip = (2 * my_ta >= n_ta) & (4 * my_sa >= 3 * n_sa)

    def all_here():
        pl.semaphore_wait(barrier, sum(count - 1 for count, _, _ in groups))

    @pl.when(last_chip)
    def _():
        all_here()
        send_norm(0)

    split_sol(*chunks[-1])

    def make_signs(lane_maps):
        for copy in small_copies:
            copy.wait()
        signs = []
        for slice_of, column in lane_maps:
            chir = jnp.ones(column.shape, jnp.float32)
            for s in range(srcs):
                for k in range(cols):
                    value = jnp.where(spin_ref[s, k] < 2, 1.0, -1.0)
                    chir = jnp.where(column // spins == s * cols + k, value, chir)
            now = my_ta * slices + slice_of
            sign = chir
            for s in range(srcs):
                value = jnp.where(now < times_ref[s], -chir, chir)
                sign = jnp.where(column // (spins * cols) == s, value, sign)
            signs.append(sign)
        return signs

    def partial(t, c):
        lanes = pl.ds(c * sites, sites)
        both = lax.dot_general(
            sol_split[t, :, lanes], eig_split[t, :, lanes], NT_DIMS,
            preferred_element_type=jnp.float32,
        )
        return both[: parts * columns] + both[parts * columns :]

    def flatten(t, p, tile):
        period = math.lcm(columns, LANES)
        rows_in, rows_out = period // columns, period // LANES
        count = eigs // rows_in
        lane = lax.broadcasted_iota(jnp.int32, (count, LANES), 1)
        tile_buf[t, p] = tile
        taken = [tile_buf[t, p, pl.ds(i, count, stride=rows_in), :] for i in range(rows_in)]
        for o in range(rows_out):
            value, filled = None, 0
            while filled < LANES:
                i, skip = divmod(o * LANES + filled, columns)
                size = min(columns - skip, LANES - filled)
                shift = (filled - skip) % LANES
                part = pltpu.roll(taken[i], shift, 1) if shift else taken[i]
                value = part if value is None else jnp.where(lane < filled, value, part)
                filled += size
            flat_buf[t, p, pl.ds(o, count, stride=rows_out), :] = value

    def store_flat(totals):
        lane = lax.broadcasted_iota(jnp.int32, (1, LANES), 1)
        signs = make_signs([(jnp.full_like(lane, t), lane) for t in range(slices)])
        for t, g in enumerate(totals):
            real, imag = jnp.transpose(g[:columns]), jnp.transpose(g[columns:])
            tiles = real[:eigs] + imag[eigs:], imag[:eigs] - real[eigs:]
            for p in range(parts):
                tile = tiles[p]
                if pad:
                    tile = jnp.concatenate([tile, jnp.zeros((eigs, pad), jnp.float32)], axis=1)
                flatten(t, p, tile * signs[t])
                for d in range(n_sa):
                    send_buf[pl.ds(d * share + t * rows + p * piece, piece), :] = flat_buf[
                        t, p, pl.ds(d * piece, piece), :
                    ]

    def store_packed(totals):
        first, second = totals
        real0, imag0 = first[:columns], first[columns:]
        real1, imag1 = second[:columns], second[columns:]
        front = lax.broadcasted_iota(jnp.int32, (1, LANES), 1) < eigs
        thirds = [slice(i * pad, (i + 1) * pad) for i in range(3)]

        def turn(body, upper, lower):
            tail = jnp.where(front, upper, lower)
            return jnp.transpose(jnp.concatenate([body, tail], axis=0))

        by_real = turn(real0, imag1[thirds[0]], real1[thirds[1]])
        by_imag = turn(imag0, imag1[thirds[1]], -real1[thirds[0]])
        by_both = turn(jnp.where(front, real1, imag1), imag1[thirds[2]], -real1[thirds[2]])
        tiles = (
            by_real[:eigs] + by_imag[eigs:],
            by_imag[:eigs] - by_real[eigs:],
            by_both[:eigs] + by_both[eigs:],
        )
        for i, tile in enumerate(tiles):
            for d in range(n_sa):
                send_buf[pl.ds(d * share + i * piece, piece), :] = tile[
                    d * piece : (d + 1) * piece
                ]

    def send_tiles():
        sent = send_buf.reshape(n_sa, share // sub, sub, LANES)
        landed = recv_buf.reshape(n_sa - 1, share // sub, sub, LANES)
        for peer, slot in others(n_sa, my_sa):
            pltpu.make_async_remote_copy(
                src_ref=sent.at[peer],
                dst_ref=landed.at[slot],
                send_sem=out_sem,
                recv_sem=in_sem,
                device_id={"sa": peer},
            ).start()

    totals = [None] * slices

    def step(c):
        for t in range(slices):
            both = partial(t, c)
            totals[t] = both if c == 0 else totals[t] + both

    for c in range(colors):
        wait_for(eig_buf.at[c], eig_sem.at[c])
        for t in range(slices):
            split_eig(t, c)
        if c:
            step(c - 1)
    step(colors - 1)
    totals = [g[:, : parts * eigs] + g[:, parts * eigs :] for g in totals]
    store_packed(totals) if packed else store_flat(totals)

    @pl.when(jnp.logical_not(last_chip))
    def _():
        all_here()
        send_norm(0)

    send_tiles()

    if len(groups) > 1:
        wait_for(norm_rows(0), norm_in_sems.at[0])
        own_norm = own_norm + jnp.sum(norm_rows(0)[...], axis=0)
        norm_send[1] = own_norm
        send_norm(1)

    lane = lax.broadcasted_iota(jnp.int32, (SUBLANES, LANES), 1)
    if packed:
        body = lane < columns
        signs = make_signs([
            (jnp.where(body, i // parts, 1), jnp.where(body, lane, lane - columns + i * pad))
            for i in range(3)
        ])
    wait_for(recv_buf, in_sem)
    total = send_buf[pl.ds(my_sa * share, share), :]
    for slot in range(n_sa - 1):
        total = total + recv_buf[pl.ds(slot * share, share), :]

    def join(pieces):
        value = None
        for start, part in pieces:
            value = part if value is None else jnp.where(lane[:1] < start, value, part)
        return value

    def put(t, p, r, value):
        out_ref[p, pl.ds(t, 1), pl.ds(r * LANES, LANES)] = value

    if packed:
        turned = {}
        for i in range(3):
            own = total[i * piece : (i + 1) * piece].reshape(-1, SUBLANES, LANES) * signs[i]
            own = own.reshape(piece, LANES)
            for shift in range(0, LANES, pad):
                turned[i, shift] = pltpu.roll(own, shift, 1) if shift else own
        for r in range(rows_own):
            starts = range(0, LANES, pad)
            from_of = [divmod(r * LANES + start, columns) for start in starts]
            for i in range(3):
                pieces = []
                for start, (row, skip) in zip(starts, from_of):
                    if not start or not skip:
                        pieces.append((start, turned[i, (start - skip) % LANES][row : row + 1]))
                put(i // parts, i % parts, r, join(pieces))
            pieces = [
                (start, turned[skip // pad, (start - columns) % LANES][row : row + 1])
                for start, (row, skip) in zip(starts, from_of)
            ]
            put(1, 1, r, join(pieces))
    else:
        for t in range(slices):
            for p in range(parts):
                for r in range(rows_own):
                    at = t * rows + p * rows_own + r
                    put(t, p, r, total[at : at + 1])
    wait_for(recv_buf, out_sem)
    for phase in range(len(groups)):
        wait_for(norm_rows(phase), norm_out_sems.at[phase])
    final = len(groups) - 1
    wait_for(norm_rows(final), norm_in_sems.at[final])
    own_norm = own_norm + jnp.sum(norm_rows(final)[...], axis=0)
    for s in range(srcs):
        row = pltpu.roll(own_norm, LANES - s * cols, 1) if s else own_norm
        norm_ref[pl.ds(s, 1), :] = row[:, :cols]


def hand_over(tiles_ref, norms_ref, out_hbm, norm_hbm, sems):
    copies = [
        pltpu.make_async_copy(tiles_ref, out_hbm, sems.at[0]),
        pltpu.make_async_copy(norms_ref, norm_hbm, sems.at[1]),
    ]
    for copy in copies:
        copy.start()
    for copy in copies:
        copy.wait()


def on_device(eigvecs, solutions, source_times, spin_dilution):
    n_ta, n_sa = lax.axis_size("ta"), lax.axis_size("sa")
    parts, slices, eigs, colors, sites = eigvecs.shape
    _, _, srcs, cols, spins, _, _ = solutions.shape
    columns = srcs * cols * spins
    width = eigs * columns // n_sa
    eig_view = jnp.transpose(eigvecs, (0, 1, 3, 2, 4))
    sol_view = jnp.transpose(solutions, (0, 1, 2, 3, 5, 4, 6)).reshape(
        parts, slices, srcs * cols, colors, spins, sites
    )
    dims = (n_ta, n_sa, parts, slices, eigs, colors, sites, srcs, cols, spins, width)
    blocks = sites // LANES
    inner = colors * sites
    share = slices * parts * (width // LANES)
    len_groups = 1 if n_ta * n_sa <= DIRECT else 2
    norm_peers = n_ta * n_sa - 1 if n_ta * n_sa <= DIRECT else n_ta + n_sa - 2
    f32, bf16 = jnp.float32, jnp.bfloat16
    dma = pltpu.SemaphoreType.DMA
    tiles, norms = pl.pallas_call(
        functools.partial(kernel, dims),
        out_shape=(
            pltpu.VMEM((parts, slices, width), f32),
            pltpu.VMEM((srcs, cols), f32),
        ),
        in_specs=[
            pl.BlockSpec(memory_space=pltpu.HBM),
            pl.BlockSpec(memory_space=pltpu.HBM),
            pl.BlockSpec(memory_space=pltpu.HBM),
            pl.BlockSpec(memory_space=pltpu.HBM),
        ],
        out_specs=(
            pl.BlockSpec(memory_space=pltpu.VMEM),
            pl.BlockSpec(memory_space=pltpu.VMEM),
        ),
        scratch_shapes=[
            pltpu.VMEM((colors, slices, parts, eigs, sites), f32),
            pltpu.VMEM((slices * colors * blocks, parts, columns, LANES), f32),
            pltpu.VMEM((slices, 2 * parts * eigs, inner), bf16),
            pltpu.VMEM((slices, 2 * parts * columns, inner), bf16),
            pltpu.VMEM((slices, parts, eigs, LANES), f32),
            pltpu.VMEM((slices, parts, eigs * columns // LANES, LANES), f32),
            pltpu.VMEM((n_sa * share, LANES), f32),
            pltpu.VMEM(((n_sa - 1) * share, LANES), f32),
            pltpu.VMEM((2, 1, LANES), f32),
            pltpu.VMEM((norm_peers, 1, LANES), f32),
            pltpu.SMEM((srcs,), jnp.int32),
            pltpu.SMEM((srcs, cols), jnp.int32),
            dma((2,)),
            dma((colors,)),
            dma((slices * colors,)),
            dma,
            dma,
            dma((len_groups,)),
            dma((len_groups,)),
        ],
        compiler_params=pltpu.CompilerParams(
            collective_id=0, has_side_effects=True, vmem_limit_bytes=66 * 10**6
        ),
    )(eig_view, sol_view, source_times, spin_dilution)
    return pl.pallas_call(
        hand_over,
        out_shape=(
            jax.ShapeDtypeStruct(tiles.shape, f32),
            jax.ShapeDtypeStruct(norms.shape, f32),
        ),
        in_specs=[pl.BlockSpec(memory_space=pltpu.VMEM)] * 2,
        out_specs=[pl.BlockSpec(memory_space=pltpu.HBM)] * 2,
        scratch_shapes=[dma((2,))],
        compiler_params=pltpu.CompilerParams(vmem_limit_bytes=2**20),
    )(tiles, norms)


def solution(mesh):
    return jax.shard_map(
        on_device,
        mesh=mesh,
        in_specs=(
            P(None, "ta", None, None, "sa"),
            P(None, "ta", None, None, None, None, "sa"),
            P(),
            P(),
        ),
        out_specs=(P(None, "ta", "sa"), P()),
        check_vma=False,
    )
```

```python
import functools
import math

import jax
import jax.numpy as jnp
from jax import lax
from jax.experimental import pallas as pl
from jax.experimental.pallas import tpu as pltpu
from jax.sharding import PartitionSpec as P

LANES = 128
SUBLANES = 8
DIRECT = 64
NT_DIMS = (((1,), (1,)), ((), ()))


def split_two(x):
    high = x.astype(jnp.bfloat16)
    low = (x - high.astype(jnp.float32)).astype(jnp.bfloat16)
    return high, low


def others(count, me):
    for k in range(count - 1):
        past = (me <= k).astype(jnp.int32)
        yield k + past, me - 1 + past


def wait_for(ref, sem):
    pltpu.make_async_copy(ref, ref, sem).wait()


def can_pack(parts, slices, eigs, columns, n_sa):
    return (
        parts == slices == 2 and parts * eigs == LANES
        and 4 * columns == 3 * LANES and eigs % (SUBLANES * n_sa) == 0
    )


def kernel(
    dims,
    eig_hbm, sol_hbm, times_hbm, spin_hbm,
    out_ref, norm_ref,
    eig_buf, sol_buf, eig_split, sol_split, tile_buf, flat_buf,
    send_buf, recv_buf, norm_send, norm_recv,
    times_ref, spin_ref, small_sem,
    eig_sem, sol_sem, out_sem, in_sem, norm_out_sems, norm_in_sems,
):
    n_ta, n_sa, parts, slices, eigs, colors, sites, srcs, cols, spins, width = dims
    columns = srcs * cols * spins
    rows_own = width // LANES
    blocks = sites // LANES
    packed = can_pack(parts, slices, eigs, columns, n_sa)
    pad = LANES - columns
    piece = eigs // n_sa if packed else rows_own
    rows = parts * rows_own
    share = 3 * piece if packed else slices * rows
    sub = math.gcd(share, SUBLANES)
    my_ta, my_sa = lax.axis_index("ta"), lax.axis_index("sa")
    barrier = pltpu.get_barrier_semaphore()

    def flat_device(at):
        return {"ta": lax.div(at, n_sa), "sa": lax.rem(at, n_sa)}

    if n_ta * n_sa <= DIRECT:
        groups = [(n_ta * n_sa, my_ta * n_sa + my_sa, flat_device)]
    else:
        groups = [
            (n_sa, my_sa, lambda at: {"sa": at}),
            (n_ta, my_ta, lambda at: {"ta": at}),
        ]
    chunks = [(t, c) for t in range(slices) for c in range(colors)]

    def read_sol(t, c):
        for j in range(blocks):
            at = (t * colors + c) * blocks + j
            pltpu.make_async_copy(
                sol_hbm.at[:, t, :, c, :, pl.ds(j * LANES, LANES)],
                sol_buf.at[at].reshape(parts, srcs * cols, spins, LANES),
                sol_sem.at[t * colors + c],
            ).start()

    ahead = len(chunks) // 2
    for t, c in chunks[:ahead]:
        read_sol(t, c)
    for count, me, device in groups:
        for peer, _ in others(count, me):
            pl.semaphore_signal(barrier, inc=1, device_id=device(peer))
    for t, c in chunks[ahead:]:
        read_sol(t, c)
    for c in range(colors):
        for t in range(slices):
            pltpu.make_async_copy(
                eig_hbm.at[:, t, c], eig_buf.at[c, t], eig_sem.at[c]
            ).start()
    small_copies = [
        pltpu.make_async_copy(times_hbm, times_ref, small_sem.at[0]),
        pltpu.make_async_copy(spin_hbm, spin_ref, small_sem.at[1]),
    ]
    for copy in small_copies:
        copy.start()

    def sol_blocks(t, c):
        for j in range(blocks):
            lanes = pl.ds(c * sites + j * LANES, LANES)
            for p in range(parts):
                yield p, lanes, sol_buf[(t * colors + c) * blocks + j, p]

    def split_sol(t, c):
        for p, lanes, x in sol_blocks(t, c):
            high, low = split_two(x)
            sol_split[t, pl.ds(p * columns, columns), lanes] = high
            sol_split[t, pl.ds((parts + p) * columns, columns), lanes] = low

    def split_eig(t, c):
        lanes = pl.ds(c * sites, sites)
        for p in range(parts):
            high, low = split_two(eig_buf[c, t, p])
            eig_split[t, pl.ds(p * eigs, eigs), lanes] = high
            eig_split[t, pl.ds((parts + p) * eigs, eigs), lanes] = low

    squares = jnp.zeros((columns, LANES), jnp.float32)
    for t, c in chunks:
        at = t * colors + c
        wait_for(sol_buf.at[pl.ds(at * blocks, blocks)], sol_sem.at[at])
        for _, _, x in sol_blocks(t, c):
            squares = squares + x * x
        if (t, c) != chunks[-1]:
            split_sol(t, c)

    cells = 1.0 * spins * colors * slices * n_ta * sites * n_sa
    sums = jnp.sum(squares, axis=1, keepdims=True) * (1.0 / cells)
    lane = lax.broadcasted_iota(jnp.int32, (columns, LANES), 1)
    group = lax.broadcasted_iota(jnp.int32, (columns, LANES), 0) // spins
    own_norm = jnp.sum(jnp.where(lane == group, sums, 0.0), axis=0, keepdims=True)

    def norm_rows(phase):
        count = groups[phase][0]
        return norm_recv.at[phase].reshape(norm_recv.shape[1], 1, LANES).at[pl.ds(0, count - 1)]

    def send_norm(phase, begin, end):
        count, me, device = groups[phase]
        rows_there = norm_recv.at[phase].reshape(norm_recv.shape[1], 1, LANES)
        for peer, slot in list(others(count, me))[begin:end]:
            pltpu.make_async_remote_copy(
                src_ref=norm_send.at[phase],
                dst_ref=rows_there.at[slot],
                send_sem=norm_out_sems.at[phase],
                recv_sem=norm_in_sems.at[phase],
                device_id=device(peer),
            ).start()

    def put_norm(phase, row):
        count = groups[phase][0]
        norm_send[phase] = row
        norm_recv[phase, pl.ds(count - 1, 1), :] = row
        for at in range(count, norm_recv.shape[1]):
            norm_recv[phase, pl.ds(at, 1), :] = jnp.zeros((1, LANES), jnp.float32)

    def all_here():
        pl.semaphore_wait(barrier, sum(count - 1 for count, _, _ in groups))

    put_norm(0, own_norm)
    norm_first = my_ta > 0

    @pl.when(norm_first)
    def _():
        all_here()
        send_norm(0, 0, None)

    split_sol(*chunks[-1])

    def make_signs(lane_maps):
        for copy in small_copies:
            copy.wait()
        signs = []
        for slice_of, column in lane_maps:
            chir = jnp.ones(column.shape, jnp.float32)
            for s in range(srcs):
                for k in range(cols):
                    value = jnp.where(spin_ref[s, k] < 2, 1.0, -1.0)
                    chir = jnp.where(column // spins == s * cols + k, value, chir)
            now = my_ta * slices + slice_of
            sign = chir
            for s in range(srcs):
                value = jnp.where(now < times_ref[s], -chir, chir)
                sign = jnp.where(column // (spins * cols) == s, value, sign)
            signs.append(sign)
        return signs

    def partial(t, c):
        lanes = pl.ds(c * sites, sites)
        both = lax.dot_general(
            sol_split[t, :, lanes], eig_split[t, :, lanes], NT_DIMS,
            preferred_element_type=jnp.float32,
        )
        return both[: parts * columns] + both[parts * columns :]

    def flatten(t, p, tile):
        period = math.lcm(columns, LANES)
        rows_in, rows_out = period // columns, period // LANES
        count = eigs // rows_in
        lane = lax.broadcasted_iota(jnp.int32, (count, LANES), 1)
        tile_buf[t, p] = tile
        taken = [tile_buf[t, p, pl.ds(i, count, stride=rows_in), :] for i in range(rows_in)]
        for o in range(rows_out):
            value, filled = None, 0
            while filled < LANES:
                i, skip = divmod(o * LANES + filled, columns)
                size = min(columns - skip, LANES - filled)
                shift = (filled - skip) % LANES
                part = pltpu.roll(taken[i], shift, 1) if shift else taken[i]
                value = part if value is None else jnp.where(lane < filled, value, part)
                filled += size
            flat_buf[t, p, pl.ds(o, count, stride=rows_out), :] = value

    def store_flat(totals):
        lane = lax.broadcasted_iota(jnp.int32, (1, LANES), 1)
        signs = make_signs([(jnp.full_like(lane, t), lane) for t in range(slices)])
        for t, g in enumerate(totals):
            real, imag = jnp.transpose(g[:columns]), jnp.transpose(g[columns:])
            tiles = real[:eigs] + imag[eigs:], imag[:eigs] - real[eigs:]
            for p in range(parts):
                tile = tiles[p]
                if pad:
                    tile = jnp.concatenate([tile, jnp.zeros((eigs, pad), jnp.float32)], axis=1)
                flatten(t, p, tile * signs[t])
                for d in range(n_sa):
                    send_buf[pl.ds(d * share + t * rows + p * piece, piece), :] = flat_buf[
                        t, p, pl.ds(d * piece, piece), :
                    ]

    def store_packed(totals):
        first, second = totals
        real0, imag0 = first[:columns], first[columns:]
        real1, imag1 = second[:columns], second[columns:]
        front = lax.broadcasted_iota(jnp.int32, (1, LANES), 1) < eigs
        thirds = [slice(i * pad, (i + 1) * pad) for i in range(3)]

        def turn(body, upper, lower):
            tail = jnp.where(front, upper, lower)
            return jnp.transpose(jnp.concatenate([body, tail], axis=0))

        by_real = turn(real0, imag1[thirds[0]], real1[thirds[1]])
        by_imag = turn(imag0, imag1[thirds[1]], -real1[thirds[0]])
        by_both = turn(jnp.where(front, real1, imag1), imag1[thirds[2]], -real1[thirds[2]])
        tiles = (
            by_real[:eigs] + by_imag[eigs:],
            by_imag[:eigs] - by_real[eigs:],
            by_both[:eigs] + by_both[eigs:],
        )
        for i, tile in enumerate(tiles):
            for d in range(n_sa):
                send_buf[pl.ds(d * share + i * piece, piece), :] = tile[
                    d * piece : (d + 1) * piece
                ]

    def send_tiles(begin, end):
        sent = send_buf.reshape(n_sa, share // sub, sub, LANES)
        landed = recv_buf.reshape(n_sa - 1, share // sub, sub, LANES)
        for peer, slot in list(others(n_sa, my_sa))[begin:end]:
            pltpu.make_async_remote_copy(
                src_ref=sent.at[peer],
                dst_ref=landed.at[slot],
                send_sem=out_sem,
                recv_sem=in_sem,
                device_id={"sa": peer},
            ).start()

    totals = [None] * slices

    def step(c):
        for t in range(slices):
            both = partial(t, c)
            totals[t] = both if c == 0 else totals[t] + both

    wait_for(eig_buf.at[0], eig_sem.at[0])
    for t in range(slices):
        split_eig(t, 0)
    for c in range(1, colors):
        wait_for(eig_buf.at[c], eig_sem.at[c])
    for c in range(colors):
        if c:
            for t in range(slices):
                split_eig(t, c)
        step(c)
    totals = [g[:, : parts * eigs] + g[:, parts * eigs :] for g in totals]
    store_packed(totals) if packed else store_flat(totals)

    @pl.when(jnp.logical_not(norm_first))
    def _():
        all_here()
        send_norm(0, 0, 2)
        send_tiles(0, 2)
        send_norm(0, 2, None)

    @pl.when(norm_first)
    def _():
        send_tiles(0, 2)

    send_tiles(2, None)

    if len(groups) > 1:
        wait_for(norm_rows(0), norm_in_sems.at[0])
        put_norm(1, jnp.sum(norm_recv[0], axis=0, keepdims=True))
        send_norm(1, 0, None)

    lane = lax.broadcasted_iota(jnp.int32, (SUBLANES, LANES), 1)
    if packed:
        body = lane < columns
        signs = make_signs([
            (jnp.where(body, i // parts, 1), jnp.where(body, lane, lane - columns + i * pad))
            for i in range(3)
        ])
    wait_for(recv_buf, in_sem)
    total = send_buf[pl.ds(my_sa * share, share), :]
    for slot in range(n_sa - 1):
        total = total + recv_buf[pl.ds(slot * share, share), :]

    def join(pieces):
        value = None
        for start, part in pieces:
            value = part if value is None else jnp.where(lane[:1] < start, value, part)
        return value

    def put(t, p, r, value):
        out_ref[p, pl.ds(t, 1), pl.ds(r * LANES, LANES)] = value

    if packed:
        turned = {}
        for i in range(3):
            own = total[i * piece : (i + 1) * piece].reshape(-1, SUBLANES, LANES) * signs[i]
            own = own.reshape(piece, LANES)
            for shift in range(0, LANES, pad):
                turned[i, shift] = pltpu.roll(own, shift, 1) if shift else own
        for r in range(rows_own):
            starts = range(0, LANES, pad)
            from_of = [divmod(r * LANES + start, columns) for start in starts]
            for i in range(3):
                pieces = []
                for start, (row, skip) in zip(starts, from_of):
                    if not start or not skip:
                        pieces.append((start, turned[i, (start - skip) % LANES][row : row + 1]))
                put(i // parts, i % parts, r, join(pieces))
            pieces = [
                (start, turned[skip // pad, (start - columns) % LANES][row : row + 1])
                for start, (row, skip) in zip(starts, from_of)
            ]
            put(1, 1, r, join(pieces))
    else:
        for t in range(slices):
            for p in range(parts):
                for r in range(rows_own):
                    at = t * rows + p * rows_own + r
                    put(t, p, r, total[at : at + 1])
    wait_for(recv_buf, out_sem)
    for phase in range(len(groups)):
        wait_for(norm_rows(phase), norm_out_sems.at[phase])
    final = len(groups) - 1
    wait_for(norm_rows(final), norm_in_sems.at[final])
    norm = jnp.sum(norm_recv[final], axis=0, keepdims=True)
    for s in range(srcs):
        row = pltpu.roll(norm, LANES - s * cols, 1) if s else norm
        norm_ref[pl.ds(s, 1), :] = row[:, :cols]


def hand_over(tiles_ref, norms_ref, out_hbm, norm_hbm, sems):
    copies = [
        pltpu.make_async_copy(tiles_ref, out_hbm, sems.at[0]),
        pltpu.make_async_copy(norms_ref, norm_hbm, sems.at[1]),
    ]
    for copy in copies:
        copy.start()
    for copy in copies:
        copy.wait()


def on_device(eigvecs, solutions, source_times, spin_dilution):
    n_ta, n_sa = lax.axis_size("ta"), lax.axis_size("sa")
    parts, slices, eigs, colors, sites = eigvecs.shape
    _, _, srcs, cols, spins, _, _ = solutions.shape
    columns = srcs * cols * spins
    width = eigs * columns // n_sa
    eig_view = jnp.transpose(eigvecs, (0, 1, 3, 2, 4))
    sol_view = jnp.transpose(solutions, (0, 1, 2, 3, 5, 4, 6)).reshape(
        parts, slices, srcs * cols, colors, spins, sites
    )
    dims = (n_ta, n_sa, parts, slices, eigs, colors, sites, srcs, cols, spins, width)
    blocks = sites // LANES
    inner = colors * sites
    share = slices * parts * (width // LANES)
    len_groups = 1 if n_ta * n_sa <= DIRECT else 2
    most = n_ta * n_sa if n_ta * n_sa <= DIRECT else max(n_ta, n_sa)
    norm_rows = pl.cdiv(most, SUBLANES) * SUBLANES
    f32, bf16 = jnp.float32, jnp.bfloat16
    dma = pltpu.SemaphoreType.DMA
    tiles, norms = pl.pallas_call(
        functools.partial(kernel, dims),
        out_shape=(
            pltpu.VMEM((parts, slices, width), f32),
            pltpu.VMEM((srcs, cols), f32),
        ),
        in_specs=[
            pl.BlockSpec(memory_space=pltpu.HBM),
            pl.BlockSpec(memory_space=pltpu.HBM),
            pl.BlockSpec(memory_space=pltpu.HBM),
            pl.BlockSpec(memory_space=pltpu.HBM),
        ],
        out_specs=(
            pl.BlockSpec(memory_space=pltpu.VMEM),
            pl.BlockSpec(memory_space=pltpu.VMEM),
        ),
        scratch_shapes=[
            pltpu.VMEM((colors, slices, parts, eigs, sites), f32),
            pltpu.VMEM((slices * colors * blocks, parts, columns, LANES), f32),
            pltpu.VMEM((slices, 2 * parts * eigs, inner), bf16),
            pltpu.VMEM((slices, 2 * parts * columns, inner), bf16),
            pltpu.VMEM((slices, parts, eigs, LANES), f32),
            pltpu.VMEM((slices, parts, eigs * columns // LANES, LANES), f32),
            pltpu.VMEM((n_sa * share, LANES), f32),
            pltpu.VMEM(((n_sa - 1) * share, LANES), f32),
            pltpu.VMEM((len_groups, 1, LANES), f32),
            pltpu.VMEM((len_groups, norm_rows, LANES), f32),
            pltpu.SMEM((srcs,), jnp.int32),
            pltpu.SMEM((srcs, cols), jnp.int32),
            dma((2,)),
            dma((colors,)),
            dma((slices * colors,)),
            dma,
            dma,
            dma((len_groups,)),
            dma((len_groups,)),
        ],
        compiler_params=pltpu.CompilerParams(
            collective_id=0, has_side_effects=True, vmem_limit_bytes=66 * 10**6
        ),
    )(eig_view, sol_view, source_times, spin_dilution)
    return pl.pallas_call(
        hand_over,
        out_shape=(
            jax.ShapeDtypeStruct(tiles.shape, f32),
            jax.ShapeDtypeStruct(norms.shape, f32),
        ),
        in_specs=[pl.BlockSpec(memory_space=pltpu.VMEM)] * 2,
        out_specs=[pl.BlockSpec(memory_space=pltpu.HBM)] * 2,
        scratch_shapes=[dma((2,))],
        compiler_params=pltpu.CompilerParams(vmem_limit_bytes=2**20),
    )(tiles, norms)


def solution(mesh):
    return jax.shard_map(
        on_device,
        mesh=mesh,
        in_specs=(
            P(None, "ta", None, None, "sa"),
            P(None, "ta", None, None, None, None, "sa"),
            P(),
            P(),
        ),
        out_specs=(P(None, "ta", "sa"), P()),
        check_vma=False,
    )
```

```python
import functools
import math

import jax
import jax.numpy as jnp
from jax import lax
from jax.experimental import pallas as pl
from jax.experimental.pallas import tpu as pltpu
from jax.sharding import PartitionSpec as P

LANES = 128
SUBLANES = 8
DIRECT = 64
NT_DIMS = (((1,), (1,)), ((), ()))


def split_two(x):
    high = x.astype(jnp.bfloat16)
    low = (x - high.astype(jnp.float32)).astype(jnp.bfloat16)
    return high, low


def others(count, me):
    for k in range(count - 1):
        past = (me <= k).astype(jnp.int32)
        yield k + past, me - 1 + past


def wait_for(ref, sem):
    pltpu.make_async_copy(ref, ref, sem).wait()


def can_pack(parts, slices, eigs, columns, n_sa):
    return (
        parts == slices == 2 and parts * eigs == LANES
        and 4 * columns == 3 * LANES and eigs % (SUBLANES * n_sa) == 0
    )


def kernel(
    dims,
    eig_hbm, sol_hbm, times_hbm, spin_hbm,
    out_ref, norm_ref,
    eig_buf, sol_buf, eig_split, sol_split, g_buf, tile_buf, flat_buf,
    send_buf, recv_buf, norm_send, norm_recv,
    times_ref, spin_ref, small_sem,
    eig_sem, sol_sem, out_sems, in_sem, norm_out_sems, norm_in_sems,
):
    n_ta, n_sa, parts, slices, eigs, colors, sites, srcs, cols, spins, width = dims
    columns = srcs * cols * spins
    rows_own = width // LANES
    blocks = sites // LANES
    packed = can_pack(parts, slices, eigs, columns, n_sa)
    pad = LANES - columns
    piece = eigs // n_sa if packed else rows_own
    rows = parts * rows_own
    share = 3 * piece if packed else slices * rows
    sub = math.gcd(share, SUBLANES)
    my_ta, my_sa = lax.axis_index("ta"), lax.axis_index("sa")
    barrier = pltpu.get_barrier_semaphore()

    def flat_device(at):
        return {"ta": lax.div(at, n_sa), "sa": lax.rem(at, n_sa)}

    if n_ta * n_sa <= DIRECT:
        groups = [(n_ta * n_sa, my_ta * n_sa + my_sa, flat_device)]
    else:
        groups = [
            (n_sa, my_sa, lambda at: {"sa": at}),
            (n_ta, my_ta, lambda at: {"ta": at}),
        ]
    chunks = [(t, c) for t in range(slices) for c in range(colors)]

    nodes = srcs * cols
    gap = (blocks + 1) * spins

    def read_sol(t, c):
        at = t * colors + c
        into = sol_buf.at[at].reshape(parts, nodes, blocks + 1, spins, LANES)
        pltpu.make_async_copy(
            sol_hbm.at[:, t, :, c], into.at[:, :, pl.ds(0, blocks)], sol_sem.at[at]
        ).start()

    ahead = len(chunks) // 2
    for t, c in chunks[:ahead]:
        read_sol(t, c)
    for count, me, device in groups:
        for peer, _ in others(count, me):
            pl.semaphore_signal(barrier, inc=1, device_id=device(peer))
    for t, c in chunks[ahead:]:
        read_sol(t, c)
    for c in range(colors):
        for t in range(slices):
            pltpu.make_async_copy(
                eig_hbm.at[:, t, c], eig_buf.at[c, t], eig_sem.at[c]
            ).start()
    small_copies = [
        pltpu.make_async_copy(times_hbm, times_ref, small_sem.at[0]),
        pltpu.make_async_copy(spin_hbm, spin_ref, small_sem.at[1]),
    ]
    for copy in small_copies:
        copy.start()

    def sol_blocks(t, c):
        at = t * colors + c
        for j in range(blocks):
            lanes = pl.ds(c * sites + j * LANES, LANES)
            for p in range(parts):
                x = [
                    sol_buf[at, p, pl.ds(j * spins + spin, nodes, stride=gap), :]
                    for spin in range(spins)
                ]
                yield p, lanes, jnp.concatenate(x, axis=0)

    def split_sol(t, c):
        for p, lanes, x in sol_blocks(t, c):
            high, low = split_two(x)
            sol_split[t, pl.ds(p * columns, columns), lanes] = high
            sol_split[t, pl.ds((parts + p) * columns, columns), lanes] = low

    def by_column(t, g):
        for p in range(parts):
            for spin in range(spins):
                start = (p * spins + spin) * nodes
                g_buf[t, pl.ds(p * columns + spin, nodes, stride=spins), :] = g[
                    start : start + nodes
                ]
        return g_buf[t]

    def split_eig(t, c):
        lanes = pl.ds(c * sites, sites)
        for p in range(parts):
            high, low = split_two(eig_buf[c, t, p])
            eig_split[t, pl.ds(p * eigs, eigs), lanes] = high
            eig_split[t, pl.ds((parts + p) * eigs, eigs), lanes] = low

    squares = jnp.zeros((columns, LANES), jnp.float32)
    for t, c in chunks:
        at = t * colors + c
        into = sol_buf.at[at].reshape(parts, nodes, blocks + 1, spins, LANES)
        wait_for(into.at[:, :, pl.ds(0, blocks)], sol_sem.at[at])
        for _, _, x in sol_blocks(t, c):
            squares = squares + x * x
        if (t, c) != chunks[-1]:
            split_sol(t, c)

    cells = 1.0 * spins * colors * slices * n_ta * sites * n_sa
    squares = sum(squares[spin * nodes : (spin + 1) * nodes] for spin in range(spins))
    sums = jnp.sum(squares, axis=1, keepdims=True) * (1.0 / cells)
    lane = lax.broadcasted_iota(jnp.int32, (nodes, LANES), 1)
    node = lax.broadcasted_iota(jnp.int32, (nodes, LANES), 0)
    own_norm = jnp.sum(jnp.where(lane == node, sums, 0.0), axis=0, keepdims=True)

    def norm_rows(phase):
        count = groups[phase][0]
        return norm_recv.at[phase].reshape(norm_recv.shape[1], 1, LANES).at[pl.ds(0, count - 1)]

    def send_norm(phase, begin, end):
        count, me, device = groups[phase]
        rows_there = norm_recv.at[phase].reshape(norm_recv.shape[1], 1, LANES)
        for peer, slot in list(others(count, me))[begin:end]:
            pltpu.make_async_remote_copy(
                src_ref=norm_send.at[phase],
                dst_ref=rows_there.at[slot],
                send_sem=norm_out_sems.at[phase],
                recv_sem=norm_in_sems.at[phase],
                device_id=device(peer),
            ).start()

    def put_norm(phase, row):
        count = groups[phase][0]
        norm_send[phase] = row
        norm_recv[phase, pl.ds(count - 1, 1), :] = row
        for at in range(count, norm_recv.shape[1]):
            norm_recv[phase, pl.ds(at, 1), :] = jnp.zeros((1, LANES), jnp.float32)

    def all_here():
        pl.semaphore_wait(barrier, sum(count - 1 for count, _, _ in groups))

    put_norm(0, own_norm)
    norm_first = my_ta > 0

    @pl.when(norm_first)
    def _():
        all_here()
        send_norm(0, 0, None)

    split_sol(*chunks[-1])

    def make_signs(lane_maps):
        for copy in small_copies:
            copy.wait()
        signs = []
        for slice_of, column in lane_maps:
            chir = jnp.ones(column.shape, jnp.float32)
            for s in range(srcs):
                for k in range(cols):
                    value = jnp.where(spin_ref[s, k] < 2, 1.0, -1.0)
                    chir = jnp.where(column // spins == s * cols + k, value, chir)
            now = my_ta * slices + slice_of
            sign = chir
            for s in range(srcs):
                value = jnp.where(now < times_ref[s], -chir, chir)
                sign = jnp.where(column // (spins * cols) == s, value, sign)
            signs.append(sign)
        return signs

    def partial(t, c):
        lanes = pl.ds(c * sites, sites)
        both = lax.dot_general(
            sol_split[t, :, lanes], eig_split[t, :, lanes], NT_DIMS,
            preferred_element_type=jnp.float32,
        )
        return both[: parts * columns] + both[parts * columns :]

    def flatten(t, p, tile):
        period = math.lcm(columns, LANES)
        rows_in, rows_out = period // columns, period // LANES
        count = eigs // rows_in
        lane = lax.broadcasted_iota(jnp.int32, (count, LANES), 1)
        tile_buf[t, p] = tile
        taken = [tile_buf[t, p, pl.ds(i, count, stride=rows_in), :] for i in range(rows_in)]
        for o in range(rows_out):
            value, filled = None, 0
            while filled < LANES:
                i, skip = divmod(o * LANES + filled, columns)
                size = min(columns - skip, LANES - filled)
                shift = (filled - skip) % LANES
                part = pltpu.roll(taken[i], shift, 1) if shift else taken[i]
                value = part if value is None else jnp.where(lane < filled, value, part)
                filled += size
            flat_buf[t, p, pl.ds(o, count, stride=rows_out), :] = value

    def store_flat(totals):
        lane = lax.broadcasted_iota(jnp.int32, (1, LANES), 1)
        signs = make_signs([(jnp.full_like(lane, t), lane) for t in range(slices)])
        for t, g in enumerate(totals):
            real, imag = jnp.transpose(g[:columns]), jnp.transpose(g[columns:])
            tiles = real[:eigs] + imag[eigs:], imag[:eigs] - real[eigs:]
            for p in range(parts):
                tile = tiles[p]
                if pad:
                    tile = jnp.concatenate([tile, jnp.zeros((eigs, pad), jnp.float32)], axis=1)
                flatten(t, p, tile * signs[t])
                for d in range(n_sa):
                    send_buf[pl.ds(d * share + t * rows + p * piece, piece), :] = flat_buf[
                        t, p, pl.ds(d * piece, piece), :
                    ]

    def store_packed(totals):
        first, second = totals
        real0, imag0 = first[:columns], first[columns:]
        real1, imag1 = second[:columns], second[columns:]
        front = lax.broadcasted_iota(jnp.int32, (1, LANES), 1) < eigs
        thirds = [slice(i * pad, (i + 1) * pad) for i in range(3)]

        def turn(body, upper, lower):
            tail = jnp.where(front, upper, lower)
            return jnp.transpose(jnp.concatenate([body, tail], axis=0))

        by_real = turn(real0, imag1[thirds[0]], real1[thirds[1]])
        by_imag = turn(imag0, imag1[thirds[1]], -real1[thirds[0]])
        by_both = turn(jnp.where(front, real1, imag1), imag1[thirds[2]], -real1[thirds[2]])
        tiles = (
            by_real[:eigs] + by_imag[eigs:],
            by_imag[:eigs] - by_real[eigs:],
            by_both[:eigs] + by_both[eigs:],
        )
        for i, tile in enumerate(tiles):
            for d in range(n_sa):
                send_buf[pl.ds(d * share + i * piece, piece), :] = tile[
                    d * piece : (d + 1) * piece
                ]

    def send_tiles(begin, end):
        sent = send_buf.reshape(n_sa, share // sub, sub, LANES)
        landed = recv_buf.reshape(n_sa - 1, share // sub, sub, LANES)
        for peer, slot in list(others(n_sa, my_sa))[begin:end]:
            pltpu.make_async_remote_copy(
                src_ref=sent.at[peer],
                dst_ref=landed.at[slot],
                send_sem=out_sems.at[min(begin, 1)],
                recv_sem=in_sem,
                device_id={"sa": peer},
            ).start()

    def first_sent():
        wait_for(recv_buf.at[pl.ds(0, 2 * share)], out_sems.at[0])

    totals = [None] * slices

    def step(c):
        for t in range(slices):
            both = partial(t, c)
            totals[t] = both if c == 0 else totals[t] + both

    wait_for(eig_buf.at[0], eig_sem.at[0])
    for t in range(slices):
        split_eig(t, 0)
    for c in range(1, colors):
        wait_for(eig_buf.at[c], eig_sem.at[c])
    for c in range(colors):
        if c:
            for t in range(slices):
                split_eig(t, c)
        step(c)
    totals = [
        by_column(t, g[:, : parts * eigs] + g[:, parts * eigs :]) for t, g in enumerate(totals)
    ]
    store_packed(totals) if packed else store_flat(totals)

    @pl.when(jnp.logical_not(norm_first))
    def _():
        all_here()
        send_norm(0, 0, 2)
        send_tiles(0, 2)
        send_norm(0, 2, None)
        first_sent()

    @pl.when(norm_first)
    def _():
        send_tiles(0, 2)
        first_sent()

    send_tiles(2, None)

    if len(groups) > 1:
        wait_for(norm_rows(0), norm_in_sems.at[0])
        put_norm(1, jnp.sum(norm_recv[0], axis=0, keepdims=True))
        send_norm(1, 0, None)

    lane = lax.broadcasted_iota(jnp.int32, (SUBLANES, LANES), 1)
    if packed:
        body = lane < columns
        signs = make_signs([
            (jnp.where(body, i // parts, 1), jnp.where(body, lane, lane - columns + i * pad))
            for i in range(3)
        ])
    wait_for(recv_buf, in_sem)
    total = send_buf[pl.ds(my_sa * share, share), :]
    for slot in range(n_sa - 1):
        total = total + recv_buf[pl.ds(slot * share, share), :]

    def join(pieces):
        value = None
        for start, part in pieces:
            value = part if value is None else jnp.where(lane[:1] < start, value, part)
        return value

    def put(t, p, r, value):
        out_ref[p, pl.ds(t, 1), pl.ds(r * LANES, LANES)] = value

    if packed:
        turned = {}
        for i in range(3):
            own = total[i * piece : (i + 1) * piece].reshape(-1, SUBLANES, LANES) * signs[i]
            own = own.reshape(piece, LANES)
            for shift in range(0, LANES, pad):
                turned[i, shift] = pltpu.roll(own, shift, 1) if shift else own
        for r in range(rows_own):
            starts = range(0, LANES, pad)
            from_of = [divmod(r * LANES + start, columns) for start in starts]
            for i in range(3):
                pieces = []
                for start, (row, skip) in zip(starts, from_of):
                    if not start or not skip:
                        pieces.append((start, turned[i, (start - skip) % LANES][row : row + 1]))
                put(i // parts, i % parts, r, join(pieces))
            pieces = [
                (start, turned[skip // pad, (start - columns) % LANES][row : row + 1])
                for start, (row, skip) in zip(starts, from_of)
            ]
            put(1, 1, r, join(pieces))
    else:
        for t in range(slices):
            for p in range(parts):
                for r in range(rows_own):
                    at = t * rows + p * rows_own + r
                    put(t, p, r, total[at : at + 1])
    wait_for(recv_buf.at[pl.ds(2 * share, (n_sa - 3) * share)], out_sems.at[1])
    for phase in range(len(groups)):
        wait_for(norm_rows(phase), norm_out_sems.at[phase])
    final = len(groups) - 1
    wait_for(norm_rows(final), norm_in_sems.at[final])
    norm = jnp.sum(norm_recv[final], axis=0, keepdims=True)
    for s in range(srcs):
        row = pltpu.roll(norm, LANES - s * cols, 1) if s else norm
        norm_ref[pl.ds(s, 1), :] = row[:, :cols]


def hand_over(tiles_ref, norms_ref, out_hbm, norm_hbm, sems):
    copies = [
        pltpu.make_async_copy(tiles_ref, out_hbm, sems.at[0]),
        pltpu.make_async_copy(norms_ref, norm_hbm, sems.at[1]),
    ]
    for copy in copies:
        copy.start()
    for copy in copies:
        copy.wait()


def on_device(eigvecs, solutions, source_times, spin_dilution):
    n_ta, n_sa = lax.axis_size("ta"), lax.axis_size("sa")
    parts, slices, eigs, colors, sites = eigvecs.shape
    _, _, srcs, cols, spins, _, _ = solutions.shape
    columns = srcs * cols * spins
    width = eigs * columns // n_sa
    eig_view = jnp.transpose(eigvecs, (0, 1, 3, 2, 4))
    sol_view = jnp.transpose(
        solutions.reshape(parts, slices, srcs * cols, spins, colors, sites // LANES, LANES),
        (0, 1, 2, 4, 5, 3, 6),
    )
    dims = (n_ta, n_sa, parts, slices, eigs, colors, sites, srcs, cols, spins, width)
    blocks = sites // LANES
    inner = colors * sites
    share = slices * parts * (width // LANES)
    len_groups = 1 if n_ta * n_sa <= DIRECT else 2
    most = n_ta * n_sa if n_ta * n_sa <= DIRECT else max(n_ta, n_sa)
    norm_rows = pl.cdiv(most, SUBLANES) * SUBLANES
    f32, bf16 = jnp.float32, jnp.bfloat16
    dma = pltpu.SemaphoreType.DMA
    tiles, norms = pl.pallas_call(
        functools.partial(kernel, dims),
        out_shape=(
            pltpu.VMEM((parts, slices, width), f32),
            pltpu.VMEM((srcs, cols), f32),
        ),
        in_specs=[
            pl.BlockSpec(memory_space=pltpu.HBM),
            pl.BlockSpec(memory_space=pltpu.HBM),
            pl.BlockSpec(memory_space=pltpu.HBM),
            pl.BlockSpec(memory_space=pltpu.HBM),
        ],
        out_specs=(
            pl.BlockSpec(memory_space=pltpu.VMEM),
            pl.BlockSpec(memory_space=pltpu.VMEM),
        ),
        scratch_shapes=[
            pltpu.VMEM((colors, slices, parts, eigs, sites), f32),
            pltpu.VMEM((slices * colors, parts, columns * (blocks + 1), LANES), f32),
            pltpu.VMEM((slices, 2 * parts * eigs, inner), bf16),
            pltpu.VMEM((slices, 2 * parts * columns, inner), bf16),
            pltpu.VMEM((slices, parts * columns, parts * eigs), f32),
            pltpu.VMEM((slices, parts, eigs, LANES), f32),
            pltpu.VMEM((slices, parts, eigs * columns // LANES, LANES), f32),
            pltpu.VMEM((n_sa * share, LANES), f32),
            pltpu.VMEM(((n_sa - 1) * share, LANES), f32),
            pltpu.VMEM((len_groups, 1, LANES), f32),
            pltpu.VMEM((len_groups, norm_rows, LANES), f32),
            pltpu.SMEM((srcs,), jnp.int32),
            pltpu.SMEM((srcs, cols), jnp.int32),
            dma((2,)),
            dma((colors,)),
            dma((slices * colors,)),
            dma((2,)),
            dma,
            dma((len_groups,)),
            dma((len_groups,)),
        ],
        compiler_params=pltpu.CompilerParams(
            collective_id=0, has_side_effects=True, vmem_limit_bytes=66 * 10**6
        ),
    )(eig_view, sol_view, source_times, spin_dilution)
    return pl.pallas_call(
        hand_over,
        out_shape=(
            jax.ShapeDtypeStruct(tiles.shape, f32),
            jax.ShapeDtypeStruct(norms.shape, f32),
        ),
        in_specs=[pl.BlockSpec(memory_space=pltpu.VMEM)] * 2,
        out_specs=[pl.BlockSpec(memory_space=pltpu.HBM)] * 2,
        scratch_shapes=[dma((2,))],
        compiler_params=pltpu.CompilerParams(vmem_limit_bytes=2**20),
    )(tiles, norms)


def solution(mesh):
    return jax.shard_map(
        on_device,
        mesh=mesh,
        in_specs=(
            P(None, "ta", None, None, "sa"),
            P(None, "ta", None, None, None, None, "sa"),
            P(),
            P(),
        ),
        out_specs=(P(None, "ta", "sa"), P()),
        check_vma=False,
    )
```

```python
import functools
import math

import jax
import jax.numpy as jnp
from jax import lax
from jax.experimental import pallas as pl
from jax.experimental.pallas import tpu as pltpu
from jax.sharding import PartitionSpec as P

LANES = 128
SUBLANES = 8
DIRECT = 64
HUBS = 2
NT_DIMS = (((1,), (1,)), ((), ()))


def split_two(x):
    high = x.astype(jnp.bfloat16)
    low = (x - high.astype(jnp.float32)).astype(jnp.bfloat16)
    return high, low


def others(count, me):
    for k in range(count - 1):
        past = (me <= k).astype(jnp.int32)
        yield k + past, me - 1 + past


def wait_for(ref, sem):
    pltpu.make_async_copy(ref, ref, sem).wait()


def can_pack(parts, slices, eigs, columns, n_sa):
    return (
        parts == slices == 2 and parts * eigs == LANES
        and 4 * columns == 3 * LANES and eigs % (SUBLANES * n_sa) == 0
    )


def kernel(
    dims,
    eig_hbm, sol_hbm, times_hbm, spin_hbm,
    out_ref, norm_ref,
    eig_buf, sol_buf, eig_split, sol_split, g_buf, tile_buf, flat_buf,
    send_buf, recv_buf, norm_send, norm_recv,
    times_ref, spin_ref, small_sem,
    eig_sem, sol_sem, out_sems, in_sem, norm_out_sems, norm_in_sems, line_sem,
):
    n_ta, n_sa, parts, slices, eigs, colors, sites, srcs, cols, spins, width = dims
    columns = srcs * cols * spins
    rows_own = width // LANES
    blocks = sites // LANES
    packed = can_pack(parts, slices, eigs, columns, n_sa)
    pad = LANES - columns
    piece = eigs // n_sa if packed else rows_own
    rows = parts * rows_own
    share = 3 * piece if packed else slices * rows
    sub = math.gcd(share, SUBLANES)
    my_ta, my_sa = lax.axis_index("ta"), lax.axis_index("sa")
    barrier = pltpu.get_barrier_semaphore()

    def flat_device(at):
        return {"ta": lax.div(at, n_sa), "sa": lax.rem(at, n_sa)}

    direct = n_ta * n_sa <= DIRECT
    lines = [
        (n_sa, my_sa, lambda at: {"sa": at}),
        (n_ta, my_ta, lambda at: {"ta": at}),
    ]
    groups = [(n_ta * n_sa, my_ta * n_sa + my_sa, flat_device)] if direct else lines
    chunks = [(t, c) for t in range(slices) for c in range(colors)]

    nodes = srcs * cols
    gap = (blocks + 1) * spins

    def read_sol(t, c):
        at = t * colors + c
        into = sol_buf.at[at].reshape(parts, nodes, blocks + 1, spins, LANES)
        pltpu.make_async_copy(
            sol_hbm.at[:, t, :, c], into.at[:, :, pl.ds(0, blocks)], sol_sem.at[at]
        ).start()

    ahead = len(chunks) // 2
    for t, c in chunks[:ahead]:
        read_sol(t, c)
    for count, me, device in lines:
        for peer, _ in others(count, me):
            pl.semaphore_signal(barrier, inc=1, device_id=device(peer))
    for t, c in chunks[ahead:]:
        read_sol(t, c)
    for c in range(colors):
        for t in range(slices):
            pltpu.make_async_copy(
                eig_hbm.at[:, t, c], eig_buf.at[c, t], eig_sem.at[c]
            ).start()
    small_copies = [
        pltpu.make_async_copy(times_hbm, times_ref, small_sem.at[0]),
        pltpu.make_async_copy(spin_hbm, spin_ref, small_sem.at[1]),
    ]
    for copy in small_copies:
        copy.start()

    expected = n_sa - 1 + n_ta - 1
    if direct:
        @pl.when((my_ta == 0) & (my_sa < HUBS))
        def _():
            for a in range(1, n_ta):
                for peer, _ in others(n_sa, my_sa):
                    pl.semaphore_signal(barrier, inc=1, device_id={"ta": a, "sa": peer})

        far_hubs = HUBS - (my_sa < HUBS).astype(jnp.int32)
        expected = expected + jnp.where(my_ta > 0, far_hubs, 0)

    def sol_blocks(t, c):
        at = t * colors + c
        for j in range(blocks):
            lanes = pl.ds(c * sites + j * LANES, LANES)
            for p in range(parts):
                x = [
                    sol_buf[at, p, pl.ds(j * spins + spin, nodes, stride=gap), :]
                    for spin in range(spins)
                ]
                yield p, lanes, jnp.concatenate(x, axis=0)

    def split_sol(t, c):
        for p, lanes, x in sol_blocks(t, c):
            high, low = split_two(x)
            sol_split[t, pl.ds(p * columns, columns), lanes] = high
            sol_split[t, pl.ds((parts + p) * columns, columns), lanes] = low

    def by_column(t, g):
        for p in range(parts):
            for spin in range(spins):
                start = (p * spins + spin) * nodes
                g_buf[t, pl.ds(p * columns + spin, nodes, stride=spins), :] = g[
                    start : start + nodes
                ]
        return g_buf[t]

    def split_eig(t, c):
        lanes = pl.ds(c * sites, sites)
        for p in range(parts):
            high, low = split_two(eig_buf[c, t, p])
            eig_split[t, pl.ds(p * eigs, eigs), lanes] = high
            eig_split[t, pl.ds((parts + p) * eigs, eigs), lanes] = low

    squares = jnp.zeros((columns, LANES), jnp.float32)
    for t, c in chunks:
        at = t * colors + c
        into = sol_buf.at[at].reshape(parts, nodes, blocks + 1, spins, LANES)
        wait_for(into.at[:, :, pl.ds(0, blocks)], sol_sem.at[at])
        for _, _, x in sol_blocks(t, c):
            squares = squares + x * x
        if (t, c) != chunks[-1]:
            split_sol(t, c)

    cells = 1.0 * spins * colors * slices * n_ta * sites * n_sa
    squares = sum(squares[spin * nodes : (spin + 1) * nodes] for spin in range(spins))
    sums = jnp.sum(squares, axis=1, keepdims=True) * (1.0 / cells)
    lane = lax.broadcasted_iota(jnp.int32, (nodes, LANES), 1)
    node = lax.broadcasted_iota(jnp.int32, (nodes, LANES), 0)
    own_norm = jnp.sum(jnp.where(lane == node, sums, 0.0), axis=0, keepdims=True)

    def norm_rows(phase):
        count = groups[phase][0]
        return norm_recv.at[phase].reshape(norm_recv.shape[1], 1, LANES).at[pl.ds(0, count - 1)]

    def send_norm(phase, begin, end):
        count, me, device = groups[phase]
        rows_there = norm_recv.at[phase].reshape(norm_recv.shape[1], 1, LANES)
        for peer, slot in list(others(count, me))[begin:end]:
            pltpu.make_async_remote_copy(
                src_ref=norm_send.at[phase],
                dst_ref=rows_there.at[slot],
                send_sem=norm_out_sems.at[phase],
                recv_sem=norm_in_sems.at[phase],
                device_id=device(peer),
            ).start()

    def put_norm(phase, row):
        count = groups[phase][0]
        norm_send[phase] = row
        norm_recv[phase, pl.ds(count - 1, 1), :] = row
        for at in range(count, norm_recv.shape[1]):
            norm_recv[phase, pl.ds(at, 1), :] = jnp.zeros((1, LANES), jnp.float32)

    def lines_here():
        pl.semaphore_wait(barrier, expected)
        send_norm(0, 0, HUBS)

    def tell_line():
        if direct:
            for peer, _ in others(n_ta, my_ta):
                pl.semaphore_signal(line_sem, inc=1, device_id={"ta": peer})

    def all_here():
        if direct:
            pl.semaphore_wait(line_sem, n_ta - 1)

    put_norm(0, own_norm)
    norm_first = my_ta > 0

    @pl.when(norm_first)
    def _():
        lines_here()
        tell_line()

    split_sol(*chunks[-1])

    def make_signs(lane_maps):
        for copy in small_copies:
            copy.wait()
        signs = []
        for slice_of, column in lane_maps:
            chir = jnp.ones(column.shape, jnp.float32)
            for s in range(srcs):
                for k in range(cols):
                    value = jnp.where(spin_ref[s, k] < 2, 1.0, -1.0)
                    chir = jnp.where(column // spins == s * cols + k, value, chir)
            now = my_ta * slices + slice_of
            sign = chir
            for s in range(srcs):
                value = jnp.where(now < times_ref[s], -chir, chir)
                sign = jnp.where(column // (spins * cols) == s, value, sign)
            signs.append(sign)
        return signs

    def partial(t, c):
        lanes = pl.ds(c * sites, sites)
        both = lax.dot_general(
            sol_split[t, :, lanes], eig_split[t, :, lanes], NT_DIMS,
            preferred_element_type=jnp.float32,
        )
        return both[: parts * columns] + both[parts * columns :]

    def flatten(t, p, tile):
        period = math.lcm(columns, LANES)
        rows_in, rows_out = period // columns, period // LANES
        count = eigs // rows_in
        lane = lax.broadcasted_iota(jnp.int32, (count, LANES), 1)
        tile_buf[t, p] = tile
        taken = [tile_buf[t, p, pl.ds(i, count, stride=rows_in), :] for i in range(rows_in)]
        for o in range(rows_out):
            value, filled = None, 0
            while filled < LANES:
                i, skip = divmod(o * LANES + filled, columns)
                size = min(columns - skip, LANES - filled)
                shift = (filled - skip) % LANES
                part = pltpu.roll(taken[i], shift, 1) if shift else taken[i]
                value = part if value is None else jnp.where(lane < filled, value, part)
                filled += size
            flat_buf[t, p, pl.ds(o, count, stride=rows_out), :] = value

    def store_flat(totals):
        lane = lax.broadcasted_iota(jnp.int32, (1, LANES), 1)
        signs = make_signs([(jnp.full_like(lane, t), lane) for t in range(slices)])
        for t, g in enumerate(totals):
            real, imag = jnp.transpose(g[:columns]), jnp.transpose(g[columns:])
            tiles = real[:eigs] + imag[eigs:], imag[:eigs] - real[eigs:]
            for p in range(parts):
                tile = tiles[p]
                if pad:
                    tile = jnp.concatenate([tile, jnp.zeros((eigs, pad), jnp.float32)], axis=1)
                flatten(t, p, tile * signs[t])
                for d in range(n_sa):
                    send_buf[pl.ds(d * share + t * rows + p * piece, piece), :] = flat_buf[
                        t, p, pl.ds(d * piece, piece), :
                    ]

    def store_packed(totals):
        first, second = totals
        real0, imag0 = first[:columns], first[columns:]
        real1, imag1 = second[:columns], second[columns:]
        front = lax.broadcasted_iota(jnp.int32, (1, LANES), 1) < eigs
        thirds = [slice(i * pad, (i + 1) * pad) for i in range(3)]

        def turn(body, upper, lower):
            tail = jnp.where(front, upper, lower)
            return jnp.transpose(jnp.concatenate([body, tail], axis=0))

        by_real = turn(real0, imag1[thirds[0]], real1[thirds[1]])
        by_imag = turn(imag0, imag1[thirds[1]], -real1[thirds[0]])
        by_both = turn(jnp.where(front, real1, imag1), imag1[thirds[2]], -real1[thirds[2]])
        tiles = (
            by_real[:eigs] + by_imag[eigs:],
            by_imag[:eigs] - by_real[eigs:],
            by_both[:eigs] + by_both[eigs:],
        )
        for i, tile in enumerate(tiles):
            for d in range(n_sa):
                send_buf[pl.ds(d * share + i * piece, piece), :] = tile[
                    d * piece : (d + 1) * piece
                ]

    def send_tiles(begin, end):
        sent = send_buf.reshape(n_sa, share // sub, sub, LANES)
        landed = recv_buf.reshape(n_sa - 1, share // sub, sub, LANES)
        for peer, slot in list(others(n_sa, my_sa))[begin:end]:
            pltpu.make_async_remote_copy(
                src_ref=sent.at[peer],
                dst_ref=landed.at[slot],
                send_sem=out_sems.at[min(begin, 1)],
                recv_sem=in_sem,
                device_id={"sa": peer},
            ).start()

    def first_sent():
        wait_for(recv_buf.at[pl.ds(0, 2 * share)], out_sems.at[0])

    totals = [None] * slices

    def step(c):
        for t in range(slices):
            both = partial(t, c)
            totals[t] = both if c == 0 else totals[t] + both

    wait_for(eig_buf.at[0], eig_sem.at[0])
    for t in range(slices):
        split_eig(t, 0)
    for c in range(1, colors):
        wait_for(eig_buf.at[c], eig_sem.at[c])
    for c in range(colors):
        if c:
            for t in range(slices):
                split_eig(t, c)
        step(c)
    totals = [
        by_column(t, g[:, : parts * eigs] + g[:, parts * eigs :]) for t, g in enumerate(totals)
    ]
    store_packed(totals) if packed else store_flat(totals)

    @pl.when(jnp.logical_not(norm_first))
    def _():
        lines_here()

    send_tiles(0, 2)

    @pl.when(jnp.logical_not(norm_first))
    def _():
        tell_line()

    all_here()
    send_norm(0, HUBS, None)
    first_sent()
    send_tiles(2, None)

    if len(groups) > 1:
        wait_for(norm_rows(0), norm_in_sems.at[0])
        put_norm(1, jnp.sum(norm_recv[0], axis=0, keepdims=True))
        send_norm(1, 0, None)

    lane = lax.broadcasted_iota(jnp.int32, (SUBLANES, LANES), 1)
    if packed:
        body = lane < columns
        signs = make_signs([
            (jnp.where(body, i // parts, 1), jnp.where(body, lane, lane - columns + i * pad))
            for i in range(3)
        ])
    wait_for(recv_buf, in_sem)
    total = send_buf[pl.ds(my_sa * share, share), :]
    for slot in range(n_sa - 1):
        total = total + recv_buf[pl.ds(slot * share, share), :]

    def join(pieces):
        value = None
        for start, part in pieces:
            value = part if value is None else jnp.where(lane[:1] < start, value, part)
        return value

    def put(t, p, r, value):
        out_ref[p, pl.ds(t, 1), pl.ds(r * LANES, LANES)] = value

    if packed:
        turned = {}
        for i in range(3):
            own = total[i * piece : (i + 1) * piece].reshape(-1, SUBLANES, LANES) * signs[i]
            own = own.reshape(piece, LANES)
            for shift in range(0, LANES, pad):
                turned[i, shift] = pltpu.roll(own, shift, 1) if shift else own
        for r in range(rows_own):
            starts = range(0, LANES, pad)
            from_of = [divmod(r * LANES + start, columns) for start in starts]
            for i in range(3):
                pieces = []
                for start, (row, skip) in zip(starts, from_of):
                    if not start or not skip:
                        pieces.append((start, turned[i, (start - skip) % LANES][row : row + 1]))
                put(i // parts, i % parts, r, join(pieces))
            pieces = [
                (start, turned[skip // pad, (start - columns) % LANES][row : row + 1])
                for start, (row, skip) in zip(starts, from_of)
            ]
            put(1, 1, r, join(pieces))
    else:
        for t in range(slices):
            for p in range(parts):
                for r in range(rows_own):
                    at = t * rows + p * rows_own + r
                    put(t, p, r, total[at : at + 1])
    wait_for(recv_buf.at[pl.ds(2 * share, (n_sa - 3) * share)], out_sems.at[1])
    for phase in range(len(groups)):
        wait_for(norm_rows(phase), norm_out_sems.at[phase])
    final = len(groups) - 1
    wait_for(norm_rows(final), norm_in_sems.at[final])
    norm = jnp.sum(norm_recv[final], axis=0, keepdims=True)
    for s in range(srcs):
        row = pltpu.roll(norm, LANES - s * cols, 1) if s else norm
        norm_ref[pl.ds(s, 1), :] = row[:, :cols]


def hand_over(tiles_ref, norms_ref, out_hbm, norm_hbm, sems):
    copies = [
        pltpu.make_async_copy(tiles_ref, out_hbm, sems.at[0]),
        pltpu.make_async_copy(norms_ref, norm_hbm, sems.at[1]),
    ]
    for copy in copies:
        copy.start()
    for copy in copies:
        copy.wait()


def on_device(eigvecs, solutions, source_times, spin_dilution):
    n_ta, n_sa = lax.axis_size("ta"), lax.axis_size("sa")
    parts, slices, eigs, colors, sites = eigvecs.shape
    _, _, srcs, cols, spins, _, _ = solutions.shape
    columns = srcs * cols * spins
    width = eigs * columns // n_sa
    eig_view = jnp.transpose(eigvecs, (0, 1, 3, 2, 4))
    sol_view = jnp.transpose(
        solutions.reshape(parts, slices, srcs * cols, spins, colors, sites // LANES, LANES),
        (0, 1, 2, 4, 5, 3, 6),
    )
    dims = (n_ta, n_sa, parts, slices, eigs, colors, sites, srcs, cols, spins, width)
    blocks = sites // LANES
    inner = colors * sites
    share = slices * parts * (width // LANES)
    len_groups = 1 if n_ta * n_sa <= DIRECT else 2
    most = n_ta * n_sa if n_ta * n_sa <= DIRECT else max(n_ta, n_sa)
    norm_rows = pl.cdiv(most, SUBLANES) * SUBLANES
    f32, bf16 = jnp.float32, jnp.bfloat16
    dma = pltpu.SemaphoreType.DMA
    tiles, norms = pl.pallas_call(
        functools.partial(kernel, dims),
        out_shape=(
            pltpu.VMEM((parts, slices, width), f32),
            pltpu.VMEM((srcs, cols), f32),
        ),
        in_specs=[
            pl.BlockSpec(memory_space=pltpu.HBM),
            pl.BlockSpec(memory_space=pltpu.HBM),
            pl.BlockSpec(memory_space=pltpu.HBM),
            pl.BlockSpec(memory_space=pltpu.HBM),
        ],
        out_specs=(
            pl.BlockSpec(memory_space=pltpu.VMEM),
            pl.BlockSpec(memory_space=pltpu.VMEM),
        ),
        scratch_shapes=[
            pltpu.VMEM((colors, slices, parts, eigs, sites), f32),
            pltpu.VMEM((slices * colors, parts, columns * (blocks + 1), LANES), f32),
            pltpu.VMEM((slices, 2 * parts * eigs, inner), bf16),
            pltpu.VMEM((slices, 2 * parts * columns, inner), bf16),
            pltpu.VMEM((slices, parts * columns, parts * eigs), f32),
            pltpu.VMEM((slices, parts, eigs, LANES), f32),
            pltpu.VMEM((slices, parts, eigs * columns // LANES, LANES), f32),
            pltpu.VMEM((n_sa * share, LANES), f32),
            pltpu.VMEM(((n_sa - 1) * share, LANES), f32),
            pltpu.VMEM((len_groups, 1, LANES), f32),
            pltpu.VMEM((len_groups, norm_rows, LANES), f32),
            pltpu.SMEM((srcs,), jnp.int32),
            pltpu.SMEM((srcs, cols), jnp.int32),
            dma((2,)),
            dma((colors,)),
            dma((slices * colors,)),
            dma((2,)),
            dma,
            dma((len_groups,)),
            dma((len_groups,)),
            pltpu.SemaphoreType.REGULAR,
        ],
        compiler_params=pltpu.CompilerParams(
            collective_id=0, has_side_effects=True, vmem_limit_bytes=66 * 10**6
        ),
    )(eig_view, sol_view, source_times, spin_dilution)
    return pl.pallas_call(
        hand_over,
        out_shape=(
            jax.ShapeDtypeStruct(tiles.shape, f32),
            jax.ShapeDtypeStruct(norms.shape, f32),
        ),
        in_specs=[pl.BlockSpec(memory_space=pltpu.VMEM)] * 2,
        out_specs=[pl.BlockSpec(memory_space=pltpu.HBM)] * 2,
        scratch_shapes=[dma((2,))],
        compiler_params=pltpu.CompilerParams(vmem_limit_bytes=2**20),
    )(tiles, norms)


def solution(mesh):
    return jax.shard_map(
        on_device,
        mesh=mesh,
        in_specs=(
            P(None, "ta", None, None, "sa"),
            P(None, "ta", None, None, None, None, "sa"),
            P(),
            P(),
        ),
        out_specs=(P(None, "ta", "sa"), P()),
        check_vma=False,
    )
```

```python
import functools
import math

import jax
import jax.numpy as jnp
from jax import lax
from jax.experimental import pallas as pl
from jax.experimental.pallas import tpu as pltpu
from jax.sharding import PartitionSpec as P

LANES = 128
SUBLANES = 8
DIRECT = 64
HUBS = 2
NT_DIMS = (((1,), (1,)), ((), ()))


def split_two(x):
    high = x.astype(jnp.bfloat16)
    low = (x - high.astype(jnp.float32)).astype(jnp.bfloat16)
    return high, low


def others(count, me):
    for k in range(count - 1):
        past = (me <= k).astype(jnp.int32)
        yield k + past, me - 1 + past


def wait_for(ref, sem):
    pltpu.make_async_copy(ref, ref, sem).wait()


def can_pack(parts, slices, eigs, columns, n_sa):
    return (
        parts == slices == 2 and parts * eigs == LANES
        and 4 * columns == 3 * LANES and eigs % (SUBLANES * n_sa) == 0
    )


def kernel(
    dims,
    eig_hbm, sol_hbm, times_hbm, spin_hbm,
    out_ref, norm_ref,
    eig_buf, sol_buf, eig_split, sol_split, g_buf, tile_buf, flat_buf,
    send_buf, recv_buf, norm_send, norm_recv,
    times_ref, spin_ref, small_sem,
    eig_sem, sol_sem, out_sems, in_sem, norm_out_sems, norm_in_sems, line_sem,
):
    n_ta, n_sa, parts, slices, eigs, colors, sites, srcs, cols, spins, width = dims
    columns = srcs * cols * spins
    rows_own = width // LANES
    blocks = sites // LANES
    packed = can_pack(parts, slices, eigs, columns, n_sa)
    pad = LANES - columns
    piece = eigs // n_sa if packed else rows_own
    rows = parts * rows_own
    share = 3 * piece if packed else slices * rows
    sub = math.gcd(share, SUBLANES)
    my_ta, my_sa = lax.axis_index("ta"), lax.axis_index("sa")
    barrier = pltpu.get_barrier_semaphore()

    def flat_device(at):
        return {"ta": lax.div(at, n_sa), "sa": lax.rem(at, n_sa)}

    direct = n_ta * n_sa <= DIRECT
    lines = [
        (n_sa, my_sa, lambda at: {"sa": at}),
        (n_ta, my_ta, lambda at: {"ta": at}),
    ]
    groups = [(n_ta * n_sa, my_ta * n_sa + my_sa, flat_device)] if direct else lines
    chunks = [(t, c) for t in range(slices) for c in range(colors)]

    nodes = srcs * cols
    gap = (blocks + 1) * spins

    def read_sol(t, c):
        at = t * colors + c
        into = sol_buf.at[at].reshape(parts, nodes, blocks + 1, spins, LANES)
        pltpu.make_async_copy(
            sol_hbm.at[:, t, :, c], into.at[:, :, pl.ds(0, blocks)], sol_sem.at[at]
        ).start()

    ahead = len(chunks) // 2
    for t, c in chunks[:ahead]:
        read_sol(t, c)
    for count, me, device in lines:
        for peer, _ in others(count, me):
            pl.semaphore_signal(barrier, inc=1, device_id=device(peer))
    for t, c in chunks[ahead:]:
        read_sol(t, c)
    for c in range(colors):
        for t in range(slices):
            pltpu.make_async_copy(
                eig_hbm.at[:, t, c], eig_buf.at[c, t], eig_sem.at[min(c, 1)]
            ).start()
    small_copies = [
        pltpu.make_async_copy(times_hbm, times_ref, small_sem.at[0]),
        pltpu.make_async_copy(spin_hbm, spin_ref, small_sem.at[1]),
    ]
    for copy in small_copies:
        copy.start()

    expected = n_sa - 1 + n_ta - 1
    if direct:
        @pl.when((my_ta == 0) & (my_sa < HUBS))
        def _():
            for a in range(1, n_ta):
                for peer, _ in others(n_sa, my_sa):
                    pl.semaphore_signal(barrier, inc=1, device_id={"ta": a, "sa": peer})

        far_hubs = HUBS - (my_sa < HUBS).astype(jnp.int32)
        expected = expected + jnp.where(my_ta > 0, far_hubs, 0)

    def sol_blocks(t, c):
        at = t * colors + c
        for j in range(blocks):
            lanes = pl.ds(c * sites + j * LANES, LANES)
            for p in range(parts):
                x = [
                    sol_buf[at, p, pl.ds(j * spins + spin, nodes, stride=gap), :]
                    for spin in range(spins)
                ]
                yield p, lanes, jnp.concatenate(x, axis=0)

    def split_sol(t, c):
        for p, lanes, x in sol_blocks(t, c):
            high, low = split_two(x)
            sol_split[t, pl.ds(p * columns, columns), lanes] = high
            sol_split[t, pl.ds((parts + p) * columns, columns), lanes] = low

    def by_column(t, g):
        for p in range(parts):
            for spin in range(spins):
                start = (p * spins + spin) * nodes
                g_buf[t, pl.ds(p * columns + spin, nodes, stride=spins), :] = g[
                    start : start + nodes
                ]
        return g_buf[t]

    def split_eig(t, c):
        lanes = pl.ds(c * sites, sites)
        for p in range(parts):
            high, low = split_two(eig_buf[c, t, p])
            eig_split[t, pl.ds(p * eigs, eigs), lanes] = high
            eig_split[t, pl.ds((parts + p) * eigs, eigs), lanes] = low

    squares = jnp.zeros((columns, LANES), jnp.float32)
    for t, c in chunks:
        at = t * colors + c
        into = sol_buf.at[at].reshape(parts, nodes, blocks + 1, spins, LANES)
        wait_for(into.at[:, :, pl.ds(0, blocks)], sol_sem.at[at])
        for _, _, x in sol_blocks(t, c):
            squares = squares + x * x
        if (t, c) != chunks[-1]:
            split_sol(t, c)

    cells = 1.0 * spins * colors * slices * n_ta * sites * n_sa
    squares = sum(squares[spin * nodes : (spin + 1) * nodes] for spin in range(spins))
    sums = jnp.sum(squares, axis=1, keepdims=True) * (1.0 / cells)
    lane = lax.broadcasted_iota(jnp.int32, (nodes, LANES), 1)
    node = lax.broadcasted_iota(jnp.int32, (nodes, LANES), 0)
    own_norm = jnp.sum(jnp.where(lane == node, sums, 0.0), axis=0, keepdims=True)

    def norm_rows(phase):
        count = groups[phase][0]
        return norm_recv.at[phase].reshape(norm_recv.shape[1], 1, LANES).at[pl.ds(0, count - 1)]

    def send_norm(phase, begin, end):
        count, me, device = groups[phase]
        rows_there = norm_recv.at[phase].reshape(norm_recv.shape[1], 1, LANES)
        for peer, slot in list(others(count, me))[begin:end]:
            pltpu.make_async_remote_copy(
                src_ref=norm_send.at[phase],
                dst_ref=rows_there.at[slot],
                send_sem=norm_out_sems.at[phase],
                recv_sem=norm_in_sems.at[phase],
                device_id=device(peer),
            ).start()

    def put_norm(phase, row):
        count = groups[phase][0]
        norm_send[phase] = row
        norm_recv[phase, pl.ds(count - 1, 1), :] = row
        for at in range(count, norm_recv.shape[1]):
            norm_recv[phase, pl.ds(at, 1), :] = jnp.zeros((1, LANES), jnp.float32)

    def lines_here():
        pl.semaphore_wait(barrier, expected)
        send_norm(0, 0, HUBS)

    def tell_line():
        if direct:
            for peer, _ in others(n_ta, my_ta):
                pl.semaphore_signal(line_sem, inc=1, device_id={"ta": peer})

    def all_here():
        if direct:
            pl.semaphore_wait(line_sem, n_ta - 1)

    put_norm(0, own_norm)
    norm_first = my_ta > 0

    @pl.when(norm_first)
    def _():
        lines_here()
        tell_line()

    split_sol(*chunks[-1])

    def make_signs(lane_maps):
        for copy in small_copies:
            copy.wait()
        signs = []
        for slice_of, column in lane_maps:
            chir = jnp.ones(column.shape, jnp.float32)
            for s in range(srcs):
                for k in range(cols):
                    value = jnp.where(spin_ref[s, k] < 2, 1.0, -1.0)
                    chir = jnp.where(column // spins == s * cols + k, value, chir)
            now = my_ta * slices + slice_of
            sign = chir
            for s in range(srcs):
                value = jnp.where(now < times_ref[s], -chir, chir)
                sign = jnp.where(column // (spins * cols) == s, value, sign)
            signs.append(sign)
        return signs

    def partial(t, c):
        lanes = pl.ds(c * sites, sites)
        both = lax.dot_general(
            sol_split[t, :, lanes], eig_split[t, :, lanes], NT_DIMS,
            preferred_element_type=jnp.float32,
        )
        return both[: parts * columns] + both[parts * columns :]

    def flatten(t, p, tile):
        period = math.lcm(columns, LANES)
        rows_in, rows_out = period // columns, period // LANES
        count = eigs // rows_in
        lane = lax.broadcasted_iota(jnp.int32, (count, LANES), 1)
        tile_buf[t, p] = tile
        taken = [tile_buf[t, p, pl.ds(i, count, stride=rows_in), :] for i in range(rows_in)]
        for o in range(rows_out):
            value, filled = None, 0
            while filled < LANES:
                i, skip = divmod(o * LANES + filled, columns)
                size = min(columns - skip, LANES - filled)
                shift = (filled - skip) % LANES
                part = pltpu.roll(taken[i], shift, 1) if shift else taken[i]
                value = part if value is None else jnp.where(lane < filled, value, part)
                filled += size
            flat_buf[t, p, pl.ds(o, count, stride=rows_out), :] = value

    def store_flat(totals):
        lane = lax.broadcasted_iota(jnp.int32, (1, LANES), 1)
        signs = make_signs([(jnp.full_like(lane, t), lane) for t in range(slices)])
        for t, g in enumerate(totals):
            real, imag = jnp.transpose(g[:columns]), jnp.transpose(g[columns:])
            tiles = real[:eigs] + imag[eigs:], imag[:eigs] - real[eigs:]
            for p in range(parts):
                tile = tiles[p]
                if pad:
                    tile = jnp.concatenate([tile, jnp.zeros((eigs, pad), jnp.float32)], axis=1)
                flatten(t, p, tile * signs[t])
                for d in range(n_sa):
                    send_buf[pl.ds(d * share + t * rows + p * piece, piece), :] = flat_buf[
                        t, p, pl.ds(d * piece, piece), :
                    ]

    def store_packed(totals):
        first, second = totals
        real0, imag0 = first[:columns], first[columns:]
        real1, imag1 = second[:columns], second[columns:]
        front = lax.broadcasted_iota(jnp.int32, (1, LANES), 1) < eigs
        thirds = [slice(i * pad, (i + 1) * pad) for i in range(3)]

        def turn(body, upper, lower):
            tail = jnp.where(front, upper, lower)
            return jnp.transpose(jnp.concatenate([body, tail], axis=0))

        by_real = turn(real0, imag1[thirds[0]], real1[thirds[1]])
        by_imag = turn(imag0, imag1[thirds[1]], -real1[thirds[0]])
        by_both = turn(jnp.where(front, real1, imag1), imag1[thirds[2]], -real1[thirds[2]])
        tiles = (
            by_real[:eigs] + by_imag[eigs:],
            by_imag[:eigs] - by_real[eigs:],
            by_both[:eigs] + by_both[eigs:],
        )
        for i, tile in enumerate(tiles):
            for d in range(n_sa):
                send_buf[pl.ds(d * share + i * piece, piece), :] = tile[
                    d * piece : (d + 1) * piece
                ]

    def send_tiles(begin, end):
        sent = send_buf.reshape(n_sa, share // sub, sub, LANES)
        landed = recv_buf.reshape(n_sa - 1, share // sub, sub, LANES)
        for peer, slot in list(others(n_sa, my_sa))[begin:end]:
            pltpu.make_async_remote_copy(
                src_ref=sent.at[peer],
                dst_ref=landed.at[slot],
                send_sem=out_sems.at[min(begin, 1)],
                recv_sem=in_sem,
                device_id={"sa": peer},
            ).start()

    def first_sent():
        wait_for(recv_buf.at[pl.ds(0, 2 * share)], out_sems.at[0])

    totals = [None] * slices

    def step(c):
        for t in range(slices):
            both = partial(t, c)
            totals[t] = both if c == 0 else totals[t] + both

    wait_for(eig_buf.at[0], eig_sem.at[0])
    for t in range(slices):
        split_eig(t, 0)
    wait_for(eig_buf.at[pl.ds(1, colors - 1)], eig_sem.at[1])
    for c in range(colors):
        if c:
            for t in range(slices):
                split_eig(t, c)
        step(c)
    totals = [
        by_column(t, g[:, : parts * eigs] + g[:, parts * eigs :]) for t, g in enumerate(totals)
    ]
    store_packed(totals) if packed else store_flat(totals)

    @pl.when(jnp.logical_not(norm_first))
    def _():
        lines_here()

    send_tiles(0, 2)

    @pl.when(jnp.logical_not(norm_first))
    def _():
        tell_line()

    all_here()
    send_norm(0, HUBS, None)
    first_sent()
    send_tiles(2, None)

    if len(groups) > 1:
        wait_for(norm_rows(0), norm_in_sems.at[0])
        put_norm(1, jnp.sum(norm_recv[0], axis=0, keepdims=True))
        send_norm(1, 0, None)

    lane = lax.broadcasted_iota(jnp.int32, (SUBLANES, LANES), 1)
    if packed:
        body = lane < columns
        signs = make_signs([
            (jnp.where(body, i // parts, 1), jnp.where(body, lane, lane - columns + i * pad))
            for i in range(3)
        ])
    wait_for(recv_buf, in_sem)
    total = send_buf[pl.ds(my_sa * share, share), :]
    for slot in range(n_sa - 1):
        total = total + recv_buf[pl.ds(slot * share, share), :]

    def join(pieces):
        value = None
        for start, part in pieces:
            value = part if value is None else jnp.where(lane[:1] < start, value, part)
        return value

    def put(t, p, r, value):
        out_ref[p, pl.ds(t, 1), pl.ds(r * LANES, LANES)] = value

    if packed:
        turned = {}
        for i in range(3):
            own = total[i * piece : (i + 1) * piece].reshape(-1, SUBLANES, LANES) * signs[i]
            own = own.reshape(piece, LANES)
            for shift in range(0, LANES, pad):
                turned[i, shift] = pltpu.roll(own, shift, 1) if shift else own
        for r in range(rows_own):
            starts = range(0, LANES, pad)
            from_of = [divmod(r * LANES + start, columns) for start in starts]
            for i in range(3):
                pieces = []
                for start, (row, skip) in zip(starts, from_of):
                    if not start or not skip:
                        pieces.append((start, turned[i, (start - skip) % LANES][row : row + 1]))
                put(i // parts, i % parts, r, join(pieces))
            pieces = [
                (start, turned[skip // pad, (start - columns) % LANES][row : row + 1])
                for start, (row, skip) in zip(starts, from_of)
            ]
            put(1, 1, r, join(pieces))
    else:
        for t in range(slices):
            for p in range(parts):
                for r in range(rows_own):
                    at = t * rows + p * rows_own + r
                    put(t, p, r, total[at : at + 1])
    wait_for(recv_buf.at[pl.ds(2 * share, (n_sa - 3) * share)], out_sems.at[1])
    for phase in range(len(groups)):
        wait_for(norm_rows(phase), norm_out_sems.at[phase])
    final = len(groups) - 1
    wait_for(norm_rows(final), norm_in_sems.at[final])
    rows_by_vreg = norm_recv[final].reshape(-1, SUBLANES, LANES)
    norm_ref[...] = jnp.sum(rows_by_vreg, axis=0)


def hand_over(tiles_ref, norms_ref, out_hbm, norm_hbm, norm_buf, sems):
    tile_copy = pltpu.make_async_copy(tiles_ref, out_hbm, sems.at[0])
    tile_copy.start()
    srcs, cols = norm_buf.shape
    norm = jnp.sum(norms_ref[...], axis=0, keepdims=True)
    for s in range(srcs):
        row = pltpu.roll(norm, LANES - s * cols, 1) if s else norm
        norm_buf[pl.ds(s, 1), :] = row[:, :cols]
    norm_copy = pltpu.make_async_copy(norm_buf, norm_hbm, sems.at[1])
    norm_copy.start()
    tile_copy.wait()
    norm_copy.wait()


def on_device(eigvecs, solutions, source_times, spin_dilution):
    n_ta, n_sa = lax.axis_size("ta"), lax.axis_size("sa")
    parts, slices, eigs, colors, sites = eigvecs.shape
    _, _, srcs, cols, spins, _, _ = solutions.shape
    columns = srcs * cols * spins
    width = eigs * columns // n_sa
    eig_view = jnp.transpose(eigvecs, (0, 1, 3, 2, 4))
    sol_view = jnp.transpose(
        solutions.reshape(parts, slices, srcs * cols, spins, colors, sites // LANES, LANES),
        (0, 1, 2, 4, 5, 3, 6),
    )
    dims = (n_ta, n_sa, parts, slices, eigs, colors, sites, srcs, cols, spins, width)
    blocks = sites // LANES
    inner = colors * sites
    share = slices * parts * (width // LANES)
    len_groups = 1 if n_ta * n_sa <= DIRECT else 2
    most = n_ta * n_sa if n_ta * n_sa <= DIRECT else max(n_ta, n_sa)
    norm_rows = pl.cdiv(most, SUBLANES) * SUBLANES
    f32, bf16 = jnp.float32, jnp.bfloat16
    dma = pltpu.SemaphoreType.DMA
    tiles, norms = pl.pallas_call(
        functools.partial(kernel, dims),
        out_shape=(
            pltpu.VMEM((parts, slices, width), f32),
            pltpu.VMEM((SUBLANES, LANES), f32),
        ),
        in_specs=[
            pl.BlockSpec(memory_space=pltpu.HBM),
            pl.BlockSpec(memory_space=pltpu.HBM),
            pl.BlockSpec(memory_space=pltpu.HBM),
            pl.BlockSpec(memory_space=pltpu.HBM),
        ],
        out_specs=(
            pl.BlockSpec(memory_space=pltpu.VMEM),
            pl.BlockSpec(memory_space=pltpu.VMEM),
        ),
        scratch_shapes=[
            pltpu.VMEM((colors, slices, parts, eigs, sites), f32),
            pltpu.VMEM((slices * colors, parts, columns * (blocks + 1), LANES), f32),
            pltpu.VMEM((slices, 2 * parts * eigs, inner), bf16),
            pltpu.VMEM((slices, 2 * parts * columns, inner), bf16),
            pltpu.VMEM((slices, parts * columns, parts * eigs), f32),
            pltpu.VMEM((slices, parts, eigs, LANES), f32),
            pltpu.VMEM((slices, parts, eigs * columns // LANES, LANES), f32),
            pltpu.VMEM((n_sa * share, LANES), f32),
            pltpu.VMEM(((n_sa - 1) * share, LANES), f32),
            pltpu.VMEM((len_groups, 1, LANES), f32),
            pltpu.VMEM((len_groups, norm_rows, LANES), f32),
            pltpu.SMEM((srcs,), jnp.int32),
            pltpu.SMEM((srcs, cols), jnp.int32),
            dma((2,)),
            dma((2,)),
            dma((slices * colors,)),
            dma((2,)),
            dma,
            dma((len_groups,)),
            dma((len_groups,)),
            pltpu.SemaphoreType.REGULAR,
        ],
        compiler_params=pltpu.CompilerParams(
            collective_id=0, has_side_effects=True, vmem_limit_bytes=66 * 10**6
        ),
    )(eig_view, sol_view, source_times, spin_dilution)
    return pl.pallas_call(
        hand_over,
        out_shape=(
            jax.ShapeDtypeStruct(tiles.shape, f32),
            jax.ShapeDtypeStruct((srcs, cols), f32),
        ),
        in_specs=[pl.BlockSpec(memory_space=pltpu.VMEM)] * 2,
        out_specs=[pl.BlockSpec(memory_space=pltpu.HBM)] * 2,
        scratch_shapes=[pltpu.VMEM((srcs, cols), f32), dma((2,))],
        compiler_params=pltpu.CompilerParams(vmem_limit_bytes=2**20),
    )(tiles, norms)


def solution(mesh):
    return jax.shard_map(
        on_device,
        mesh=mesh,
        in_specs=(
            P(None, "ta", None, None, "sa"),
            P(None, "ta", None, None, None, None, "sa"),
            P(),
            P(),
        ),
        out_specs=(P(None, "ta", "sa"), P()),
        check_vma=False,
    )
```

```python
import functools
import math

import jax
import jax.numpy as jnp
from jax import lax
from jax.experimental import pallas as pl
from jax.experimental.pallas import tpu as pltpu
from jax.sharding import PartitionSpec as P

LANES = 128
SUBLANES = 8
DIRECT = 64
HUBS = 2
LATE_SPLITS = 3
NT_DIMS = (((1,), (1,)), ((), ()))


def split_two(x):
    high = x.astype(jnp.bfloat16)
    low = (x - high.astype(jnp.float32)).astype(jnp.bfloat16)
    return high, low


def others(count, me):
    for k in range(count - 1):
        past = (me <= k).astype(jnp.int32)
        yield k + past, me - 1 + past


def wait_for(ref, sem):
    pltpu.make_async_copy(ref, ref, sem).wait()


def can_pack(parts, slices, eigs, columns, n_sa):
    return (
        parts == slices == 2 and parts * eigs == LANES
        and 4 * columns == 3 * LANES and eigs % (SUBLANES * n_sa) == 0
    )


def kernel(
    dims,
    eig_hbm, sol_hbm, times_hbm, spin_hbm,
    out_ref, norm_ref,
    eig_buf, sol_buf, eig_split, sol_split, g_buf, tile_buf, flat_buf,
    send_buf, recv_buf, norm_send, norm_recv,
    times_ref, spin_ref, small_sem,
    eig_sem, sol_sem, out_sems, in_sem, norm_out_sems, norm_in_sems, line_sem,
):
    n_ta, n_sa, parts, slices, eigs, colors, sites, srcs, cols, spins, width = dims
    columns = srcs * cols * spins
    rows_own = width // LANES
    blocks = sites // LANES
    packed = can_pack(parts, slices, eigs, columns, n_sa)
    pad = LANES - columns
    piece = eigs // n_sa if packed else rows_own
    rows = parts * rows_own
    share = 3 * piece if packed else slices * rows
    sub = math.gcd(share, SUBLANES)
    my_ta, my_sa = lax.axis_index("ta"), lax.axis_index("sa")
    barrier = pltpu.get_barrier_semaphore()

    def flat_device(at):
        return {"ta": lax.div(at, n_sa), "sa": lax.rem(at, n_sa)}

    direct = n_ta * n_sa <= DIRECT
    lines = [
        (n_sa, my_sa, lambda at: {"sa": at}),
        (n_ta, my_ta, lambda at: {"ta": at}),
    ]
    groups = [(n_ta * n_sa, my_ta * n_sa + my_sa, flat_device)] if direct else lines
    chunks = [(t, c) for t in range(slices) for c in range(colors)]

    nodes = srcs * cols
    gap = (blocks + 1) * spins

    def read_sol(t, c):
        at = t * colors + c
        into = sol_buf.at[at].reshape(parts, nodes, blocks + 1, spins, LANES)
        pltpu.make_async_copy(
            sol_hbm.at[:, t, :, c], into.at[:, :, pl.ds(0, blocks)], sol_sem.at[at]
        ).start()

    ahead = len(chunks) // 2
    for t, c in chunks[:ahead]:
        read_sol(t, c)
    for count, me, device in lines:
        for peer, _ in others(count, me):
            pl.semaphore_signal(barrier, inc=1, device_id=device(peer))
    for t, c in chunks[ahead:]:
        read_sol(t, c)
    for c in range(colors):
        for t in range(slices):
            pltpu.make_async_copy(
                eig_hbm.at[:, t, c], eig_buf.at[c, t], eig_sem.at[min(c, 1)]
            ).start()
    small_copies = [
        pltpu.make_async_copy(times_hbm, times_ref, small_sem.at[0]),
        pltpu.make_async_copy(spin_hbm, spin_ref, small_sem.at[1]),
    ]
    for copy in small_copies:
        copy.start()

    expected = n_sa - 1 + n_ta - 1
    if direct:
        @pl.when((my_ta == 0) & (my_sa < HUBS))
        def _():
            for a in range(1, n_ta):
                for peer, _ in others(n_sa, my_sa):
                    pl.semaphore_signal(barrier, inc=1, device_id={"ta": a, "sa": peer})

        far_hubs = HUBS - (my_sa < HUBS).astype(jnp.int32)
        expected = expected + jnp.where(my_ta > 0, far_hubs, 0)

    def sol_blocks(t, c):
        at = t * colors + c
        for j in range(blocks):
            lanes = pl.ds(c * sites + j * LANES, LANES)
            for p in range(parts):
                x = [
                    sol_buf[at, p, pl.ds(j * spins + spin, nodes, stride=gap), :]
                    for spin in range(spins)
                ]
                yield p, lanes, jnp.concatenate(x, axis=0)

    def split_sol(t, c):
        for p, lanes, x in sol_blocks(t, c):
            high, low = split_two(x)
            sol_split[t, pl.ds(p * columns, columns), lanes] = high
            sol_split[t, pl.ds((parts + p) * columns, columns), lanes] = low

    def by_column(t, g):
        for p in range(parts):
            for spin in range(spins):
                start = (p * spins + spin) * nodes
                g_buf[t, pl.ds(p * columns + spin, nodes, stride=spins), :] = g[
                    start : start + nodes
                ]
        return g_buf[t]

    def split_eig(t, c):
        lanes = pl.ds(c * sites, sites)
        for p in range(parts):
            high, low = split_two(eig_buf[c, t, p])
            eig_split[t, pl.ds(p * eigs, eigs), lanes] = high
            eig_split[t, pl.ds((parts + p) * eigs, eigs), lanes] = low

    squares = jnp.zeros((columns, LANES), jnp.float32)
    for t, c in chunks:
        at = t * colors + c
        into = sol_buf.at[at].reshape(parts, nodes, blocks + 1, spins, LANES)
        wait_for(into.at[:, :, pl.ds(0, blocks)], sol_sem.at[at])
        for _, _, x in sol_blocks(t, c):
            squares = squares + x * x
        if (t, c) not in chunks[-LATE_SPLITS:]:
            split_sol(t, c)

    cells = 1.0 * spins * colors * slices * n_ta * sites * n_sa
    squares = sum(squares[spin * nodes : (spin + 1) * nodes] for spin in range(spins))
    sums = jnp.sum(squares, axis=1, keepdims=True) * (1.0 / cells)
    lane = lax.broadcasted_iota(jnp.int32, (nodes, LANES), 1)
    node = lax.broadcasted_iota(jnp.int32, (nodes, LANES), 0)
    own_norm = jnp.sum(jnp.where(lane == node, sums, 0.0), axis=0, keepdims=True)

    def norm_rows(phase):
        count = groups[phase][0]
        return norm_recv.at[phase].reshape(norm_recv.shape[1], 1, LANES).at[pl.ds(0, count - 1)]

    def send_norm(phase, begin, end):
        count, me, device = groups[phase]
        rows_there = norm_recv.at[phase].reshape(norm_recv.shape[1], 1, LANES)
        for peer, slot in list(others(count, me))[begin:end]:
            pltpu.make_async_remote_copy(
                src_ref=norm_send.at[phase],
                dst_ref=rows_there.at[slot],
                send_sem=norm_out_sems.at[phase],
                recv_sem=norm_in_sems.at[phase],
                device_id=device(peer),
            ).start()

    def put_norm(phase, row):
        count = groups[phase][0]
        norm_send[phase] = row
        norm_recv[phase, pl.ds(count - 1, 1), :] = row
        for at in range(count, norm_recv.shape[1]):
            norm_recv[phase, pl.ds(at, 1), :] = jnp.zeros((1, LANES), jnp.float32)

    def lines_here():
        pl.semaphore_wait(barrier, expected)
        send_norm(0, 0, HUBS)

    def tell_line():
        if direct:
            for peer, _ in others(n_ta, my_ta):
                pl.semaphore_signal(line_sem, inc=1, device_id={"ta": peer})

    def all_here():
        if direct:
            pl.semaphore_wait(line_sem, n_ta - 1)

    put_norm(0, own_norm)
    norm_first = my_ta > 0

    @pl.when(norm_first)
    def _():
        lines_here()
        tell_line()

    for t, c in chunks[-LATE_SPLITS:]:
        split_sol(t, c)

    def make_signs(lane_maps):
        for copy in small_copies:
            copy.wait()
        signs = []
        for slice_of, column in lane_maps:
            chir = jnp.ones(column.shape, jnp.float32)
            for s in range(srcs):
                for k in range(cols):
                    value = jnp.where(spin_ref[s, k] < 2, 1.0, -1.0)
                    chir = jnp.where(column // spins == s * cols + k, value, chir)
            now = my_ta * slices + slice_of
            sign = chir
            for s in range(srcs):
                value = jnp.where(now < times_ref[s], -chir, chir)
                sign = jnp.where(column // (spins * cols) == s, value, sign)
            signs.append(sign)
        return signs

    def partial(t, c):
        lanes = pl.ds(c * sites, sites)
        both = lax.dot_general(
            sol_split[t, :, lanes], eig_split[t, :, lanes], NT_DIMS,
            preferred_element_type=jnp.float32,
        )
        return both[: parts * columns] + both[parts * columns :]

    def flatten(t, p, tile):
        period = math.lcm(columns, LANES)
        rows_in, rows_out = period // columns, period // LANES
        count = eigs // rows_in
        lane = lax.broadcasted_iota(jnp.int32, (count, LANES), 1)
        tile_buf[t, p] = tile
        taken = [tile_buf[t, p, pl.ds(i, count, stride=rows_in), :] for i in range(rows_in)]
        for o in range(rows_out):
            value, filled = None, 0
            while filled < LANES:
                i, skip = divmod(o * LANES + filled, columns)
                size = min(columns - skip, LANES - filled)
                shift = (filled - skip) % LANES
                part = pltpu.roll(taken[i], shift, 1) if shift else taken[i]
                value = part if value is None else jnp.where(lane < filled, value, part)
                filled += size
            flat_buf[t, p, pl.ds(o, count, stride=rows_out), :] = value

    def store_flat(totals):
        lane = lax.broadcasted_iota(jnp.int32, (1, LANES), 1)
        signs = make_signs([(jnp.full_like(lane, t), lane) for t in range(slices)])
        for t, g in enumerate(totals):
            real, imag = jnp.transpose(g[:columns]), jnp.transpose(g[columns:])
            tiles = real[:eigs] + imag[eigs:], imag[:eigs] - real[eigs:]
            for p in range(parts):
                tile = tiles[p]
                if pad:
                    tile = jnp.concatenate([tile, jnp.zeros((eigs, pad), jnp.float32)], axis=1)
                flatten(t, p, tile * signs[t])
                for d in range(n_sa):
                    send_buf[pl.ds(d * share + t * rows + p * piece, piece), :] = flat_buf[
                        t, p, pl.ds(d * piece, piece), :
                    ]

    def store_packed(totals):
        first, second = totals
        real0, imag0 = first[:columns], first[columns:]
        real1, imag1 = second[:columns], second[columns:]
        front = lax.broadcasted_iota(jnp.int32, (1, LANES), 1) < eigs
        thirds = [slice(i * pad, (i + 1) * pad) for i in range(3)]

        def turn(body, upper, lower):
            tail = jnp.where(front, upper, lower)
            return jnp.transpose(jnp.concatenate([body, tail], axis=0))

        by_real = turn(real0, imag1[thirds[0]], real1[thirds[1]])
        by_imag = turn(imag0, imag1[thirds[1]], -real1[thirds[0]])
        by_both = turn(jnp.where(front, real1, imag1), imag1[thirds[2]], -real1[thirds[2]])
        tiles = (
            by_real[:eigs] + by_imag[eigs:],
            by_imag[:eigs] - by_real[eigs:],
            by_both[:eigs] + by_both[eigs:],
        )
        for i, tile in enumerate(tiles):
            for d in range(n_sa):
                send_buf[pl.ds(d * share + i * piece, piece), :] = tile[
                    d * piece : (d + 1) * piece
                ]

    def send_tiles(begin, end):
        sent = send_buf.reshape(n_sa, share // sub, sub, LANES)
        landed = recv_buf.reshape(n_sa - 1, share // sub, sub, LANES)
        for peer, slot in list(others(n_sa, my_sa))[begin:end]:
            pltpu.make_async_remote_copy(
                src_ref=sent.at[peer],
                dst_ref=landed.at[slot],
                send_sem=out_sems.at[min(begin, 1)],
                recv_sem=in_sem,
                device_id={"sa": peer},
            ).start()

    def first_sent():
        wait_for(recv_buf.at[pl.ds(0, 2 * share)], out_sems.at[0])

    totals = [None] * slices

    def step(c):
        for t in range(slices):
            both = partial(t, c)
            totals[t] = both if c == 0 else totals[t] + both

    wait_for(eig_buf.at[0], eig_sem.at[0])
    for t in range(slices):
        split_eig(t, 0)
    wait_for(eig_buf.at[pl.ds(1, colors - 1)], eig_sem.at[1])
    for c in range(colors):
        if c:
            for t in range(slices):
                split_eig(t, c)
        step(c)
    totals = [
        by_column(t, g[:, : parts * eigs] + g[:, parts * eigs :]) for t, g in enumerate(totals)
    ]
    store_packed(totals) if packed else store_flat(totals)

    @pl.when(jnp.logical_not(norm_first))
    def _():
        lines_here()

    send_tiles(0, 2)

    @pl.when(jnp.logical_not(norm_first))
    def _():
        tell_line()

    all_here()
    send_norm(0, HUBS, None)
    first_sent()
    send_tiles(2, None)

    if len(groups) > 1:
        wait_for(norm_rows(0), norm_in_sems.at[0])
        put_norm(1, jnp.sum(norm_recv[0], axis=0, keepdims=True))
        send_norm(1, 0, None)

    lane = lax.broadcasted_iota(jnp.int32, (SUBLANES, LANES), 1)
    if packed:
        body = lane < columns
        signs = make_signs([
            (jnp.where(body, i // parts, 1), jnp.where(body, lane, lane - columns + i * pad))
            for i in range(3)
        ])
    wait_for(recv_buf, in_sem)
    total = send_buf[pl.ds(my_sa * share, share), :]
    for slot in range(n_sa - 1):
        total = total + recv_buf[pl.ds(slot * share, share), :]

    def join(pieces):
        value = None
        for start, part in pieces:
            value = part if value is None else jnp.where(lane[:1] < start, value, part)
        return value

    def put(t, p, r, value):
        out_ref[p, pl.ds(t, 1), pl.ds(r * LANES, LANES)] = value

    if packed:
        turned = {}
        for i in range(3):
            own = total[i * piece : (i + 1) * piece].reshape(-1, SUBLANES, LANES) * signs[i]
            own = own.reshape(piece, LANES)
            for shift in range(0, LANES, pad):
                turned[i, shift] = pltpu.roll(own, shift, 1) if shift else own
        for r in range(rows_own):
            starts = range(0, LANES, pad)
            from_of = [divmod(r * LANES + start, columns) for start in starts]
            for i in range(3):
                pieces = []
                for start, (row, skip) in zip(starts, from_of):
                    if not start or not skip:
                        pieces.append((start, turned[i, (start - skip) % LANES][row : row + 1]))
                put(i // parts, i % parts, r, join(pieces))
            pieces = [
                (start, turned[skip // pad, (start - columns) % LANES][row : row + 1])
                for start, (row, skip) in zip(starts, from_of)
            ]
            put(1, 1, r, join(pieces))
    else:
        for t in range(slices):
            for p in range(parts):
                for r in range(rows_own):
                    at = t * rows + p * rows_own + r
                    put(t, p, r, total[at : at + 1])
    wait_for(recv_buf.at[pl.ds(2 * share, (n_sa - 3) * share)], out_sems.at[1])
    for phase in range(len(groups)):
        wait_for(norm_rows(phase), norm_out_sems.at[phase])
    final = len(groups) - 1
    wait_for(norm_rows(final), norm_in_sems.at[final])
    rows_by_vreg = norm_recv[final].reshape(-1, SUBLANES, LANES)
    norm_ref[...] = jnp.sum(rows_by_vreg, axis=0)


def hand_over(tiles_ref, norms_ref, out_hbm, norm_hbm, norm_buf, sems):
    tile_copy = pltpu.make_async_copy(tiles_ref, out_hbm, sems.at[0])
    tile_copy.start()
    srcs, cols = norm_buf.shape
    norm = jnp.sum(norms_ref[...], axis=0, keepdims=True)
    for s in range(srcs):
        row = pltpu.roll(norm, LANES - s * cols, 1) if s else norm
        norm_buf[pl.ds(s, 1), :] = row[:, :cols]
    norm_copy = pltpu.make_async_copy(norm_buf, norm_hbm, sems.at[1])
    norm_copy.start()
    tile_copy.wait()
    norm_copy.wait()


def on_device(eigvecs, solutions, source_times, spin_dilution):
    n_ta, n_sa = lax.axis_size("ta"), lax.axis_size("sa")
    parts, slices, eigs, colors, sites = eigvecs.shape
    _, _, srcs, cols, spins, _, _ = solutions.shape
    columns = srcs * cols * spins
    width = eigs * columns // n_sa
    eig_view = jnp.transpose(eigvecs, (0, 1, 3, 2, 4))
    sol_view = jnp.transpose(
        solutions.reshape(parts, slices, srcs * cols, spins, colors, sites // LANES, LANES),
        (0, 1, 2, 4, 5, 3, 6),
    )
    dims = (n_ta, n_sa, parts, slices, eigs, colors, sites, srcs, cols, spins, width)
    blocks = sites // LANES
    inner = colors * sites
    share = slices * parts * (width // LANES)
    len_groups = 1 if n_ta * n_sa <= DIRECT else 2
    most = n_ta * n_sa if n_ta * n_sa <= DIRECT else max(n_ta, n_sa)
    norm_rows = pl.cdiv(most, SUBLANES) * SUBLANES
    f32, bf16 = jnp.float32, jnp.bfloat16
    dma = pltpu.SemaphoreType.DMA
    tiles, norms = pl.pallas_call(
        functools.partial(kernel, dims),
        out_shape=(
            pltpu.VMEM((parts, slices, width), f32),
            pltpu.VMEM((SUBLANES, LANES), f32),
        ),
        in_specs=[
            pl.BlockSpec(memory_space=pltpu.HBM),
            pl.BlockSpec(memory_space=pltpu.HBM),
            pl.BlockSpec(memory_space=pltpu.HBM),
            pl.BlockSpec(memory_space=pltpu.HBM),
        ],
        out_specs=(
            pl.BlockSpec(memory_space=pltpu.VMEM),
            pl.BlockSpec(memory_space=pltpu.VMEM),
        ),
        scratch_shapes=[
            pltpu.VMEM((colors, slices, parts, eigs, sites), f32),
            pltpu.VMEM((slices * colors, parts, columns * (blocks + 1), LANES), f32),
            pltpu.VMEM((slices, 2 * parts * eigs, inner), bf16),
            pltpu.VMEM((slices, 2 * parts * columns, inner), bf16),
            pltpu.VMEM((slices, parts * columns, parts * eigs), f32),
            pltpu.VMEM((slices, parts, eigs, LANES), f32),
            pltpu.VMEM((slices, parts, eigs * columns // LANES, LANES), f32),
            pltpu.VMEM((n_sa * share, LANES), f32),
            pltpu.VMEM(((n_sa - 1) * share, LANES), f32),
            pltpu.VMEM((len_groups, 1, LANES), f32),
            pltpu.VMEM((len_groups, norm_rows, LANES), f32),
            pltpu.SMEM((srcs,), jnp.int32),
            pltpu.SMEM((srcs, cols), jnp.int32),
            dma((2,)),
            dma((2,)),
            dma((slices * colors,)),
            dma((2,)),
            dma,
            dma((len_groups,)),
            dma((len_groups,)),
            pltpu.SemaphoreType.REGULAR,
        ],
        compiler_params=pltpu.CompilerParams(
            collective_id=0, has_side_effects=True, vmem_limit_bytes=66 * 10**6
        ),
    )(eig_view, sol_view, source_times, spin_dilution)
    return pl.pallas_call(
        hand_over,
        out_shape=(
            jax.ShapeDtypeStruct(tiles.shape, f32),
            jax.ShapeDtypeStruct((srcs, cols), f32),
        ),
        in_specs=[pl.BlockSpec(memory_space=pltpu.VMEM)] * 2,
        out_specs=[pl.BlockSpec(memory_space=pltpu.HBM)] * 2,
        scratch_shapes=[pltpu.VMEM((srcs, cols), f32), dma((2,))],
        compiler_params=pltpu.CompilerParams(vmem_limit_bytes=2**20),
    )(tiles, norms)


def solution(mesh):
    return jax.shard_map(
        on_device,
        mesh=mesh,
        in_specs=(
            P(None, "ta", None, None, "sa"),
            P(None, "ta", None, None, None, None, "sa"),
            P(),
            P(),
        ),
        out_specs=(P(None, "ta", "sa"), P()),
        check_vma=False,
    )
```

```python
import functools
import math

import jax
import jax.numpy as jnp
from jax import lax
from jax.experimental import pallas as pl
from jax.experimental.pallas import tpu as pltpu
from jax.sharding import PartitionSpec as P

LANES = 128
SUBLANES = 8
DIRECT = 64
HUBS = 2
LATE_SPLITS = 4
NT_DIMS = (((1,), (1,)), ((), ()))


def split_two(x):
    high = x.astype(jnp.bfloat16)
    low = (x - high.astype(jnp.float32)).astype(jnp.bfloat16)
    return high, low


def others(count, me):
    for k in range(count - 1):
        past = (me <= k).astype(jnp.int32)
        yield k + past, me - 1 + past


def wait_for(ref, sem):
    pltpu.make_async_copy(ref, ref, sem).wait()


def can_pack(parts, slices, eigs, columns, n_sa):
    return (
        parts == slices == 2 and parts * eigs == LANES
        and 4 * columns == 3 * LANES and eigs % (SUBLANES * n_sa) == 0
    )


def kernel(
    dims,
    eig_hbm, sol_hbm, times_hbm, spin_hbm,
    out_ref, norm_ref,
    eig_buf, sol_buf, eig_split, sol_split, g_buf, tile_buf, flat_buf,
    send_buf, recv_buf, norm_send, norm_recv,
    times_ref, spin_ref, small_sem,
    eig_sem, sol_sem, out_sems, in_sem, norm_out_sems, norm_in_sems, line_sem,
):
    n_ta, n_sa, parts, slices, eigs, colors, sites, srcs, cols, spins, width = dims
    columns = srcs * cols * spins
    rows_own = width // LANES
    blocks = sites // LANES
    packed = can_pack(parts, slices, eigs, columns, n_sa)
    pad = LANES - columns
    piece = eigs // n_sa if packed else rows_own
    rows = parts * rows_own
    share = 3 * piece if packed else slices * rows
    sub = math.gcd(share, SUBLANES)
    my_ta, my_sa = lax.axis_index("ta"), lax.axis_index("sa")
    barrier = pltpu.get_barrier_semaphore()

    def flat_device(at):
        return {"ta": lax.div(at, n_sa), "sa": lax.rem(at, n_sa)}

    direct = n_ta * n_sa <= DIRECT
    lines = [
        (n_sa, my_sa, lambda at: {"sa": at}),
        (n_ta, my_ta, lambda at: {"ta": at}),
    ]
    groups = [(n_ta * n_sa, my_ta * n_sa + my_sa, flat_device)] if direct else lines
    chunks = [(t, c) for t in range(slices) for c in range(colors)]

    nodes = srcs * cols
    gap = (blocks + 1) * spins

    def read_sol(t, c):
        at = t * colors + c
        into = sol_buf.at[at].reshape(parts, nodes, blocks + 1, spins, LANES)
        pltpu.make_async_copy(
            sol_hbm.at[:, t, :, c], into.at[:, :, pl.ds(0, blocks)], sol_sem.at[at]
        ).start()

    ahead = len(chunks)
    for t, c in chunks[:ahead]:
        read_sol(t, c)
    for count, me, device in lines:
        for peer, _ in others(count, me):
            pl.semaphore_signal(barrier, inc=1, device_id=device(peer))
    for t, c in chunks[ahead:]:
        read_sol(t, c)
    for c in range(colors):
        for t in range(slices):
            pltpu.make_async_copy(
                eig_hbm.at[:, t, c], eig_buf.at[c, t], eig_sem.at[min(c, 1)]
            ).start()
    small_copies = [
        pltpu.make_async_copy(times_hbm, times_ref, small_sem.at[0]),
        pltpu.make_async_copy(spin_hbm, spin_ref, small_sem.at[1]),
    ]
    for copy in small_copies:
        copy.start()

    expected = n_sa - 1 + n_ta - 1
    if direct:
        @pl.when((my_ta == 0) & (my_sa < HUBS))
        def _():
            for a in range(1, n_ta):
                for peer, _ in others(n_sa, my_sa):
                    pl.semaphore_signal(barrier, inc=1, device_id={"ta": a, "sa": peer})

        far_hubs = HUBS - (my_sa < HUBS).astype(jnp.int32)
        expected = expected + jnp.where(my_ta > 0, far_hubs, 0)

    def sol_blocks(t, c):
        at = t * colors + c
        for j in range(blocks):
            lanes = pl.ds(c * sites + j * LANES, LANES)
            for p in range(parts):
                x = [
                    sol_buf[at, p, pl.ds(j * spins + spin, nodes, stride=gap), :]
                    for spin in range(spins)
                ]
                yield p, lanes, jnp.concatenate(x, axis=0)

    def split_sol(t, c):
        for p, lanes, x in sol_blocks(t, c):
            high, low = split_two(x)
            sol_split[t, pl.ds(p * columns, columns), lanes] = high
            sol_split[t, pl.ds((parts + p) * columns, columns), lanes] = low

    def by_column(t, g):
        for p in range(parts):
            for spin in range(spins):
                start = (p * spins + spin) * nodes
                g_buf[t, pl.ds(p * columns + spin, nodes, stride=spins), :] = g[
                    start : start + nodes
                ]
        return g_buf[t]

    def split_eig(t, c):
        lanes = pl.ds(c * sites, sites)
        for p in range(parts):
            high, low = split_two(eig_buf[c, t, p])
            eig_split[t, pl.ds(p * eigs, eigs), lanes] = high
            eig_split[t, pl.ds((parts + p) * eigs, eigs), lanes] = low

    squares = jnp.zeros((columns, LANES), jnp.float32)
    for t, c in chunks:
        at = t * colors + c
        into = sol_buf.at[at].reshape(parts, nodes, blocks + 1, spins, LANES)
        wait_for(into.at[:, :, pl.ds(0, blocks)], sol_sem.at[at])
        for _, _, x in sol_blocks(t, c):
            squares = squares + x * x
        if (t, c) not in chunks[-LATE_SPLITS:]:
            split_sol(t, c)

    cells = 1.0 * spins * colors * slices * n_ta * sites * n_sa
    squares = sum(squares[spin * nodes : (spin + 1) * nodes] for spin in range(spins))
    sums = jnp.sum(squares, axis=1, keepdims=True) * (1.0 / cells)
    lane = lax.broadcasted_iota(jnp.int32, (nodes, LANES), 1)
    node = lax.broadcasted_iota(jnp.int32, (nodes, LANES), 0)
    own_norm = jnp.sum(jnp.where(lane == node, sums, 0.0), axis=0, keepdims=True)

    def norm_rows(phase):
        count = groups[phase][0]
        return norm_recv.at[phase].reshape(norm_recv.shape[1], 1, LANES).at[pl.ds(0, count - 1)]

    def send_norm(phase, begin, end):
        count, me, device = groups[phase]
        rows_there = norm_recv.at[phase].reshape(norm_recv.shape[1], 1, LANES)
        for peer, slot in list(others(count, me))[begin:end]:
            pltpu.make_async_remote_copy(
                src_ref=norm_send.at[phase],
                dst_ref=rows_there.at[slot],
                send_sem=norm_out_sems.at[phase],
                recv_sem=norm_in_sems.at[phase],
                device_id=device(peer),
            ).start()

    def put_norm(phase, row):
        count = groups[phase][0]
        norm_send[phase] = row
        norm_recv[phase, pl.ds(count - 1, 1), :] = row
        for at in range(count, norm_recv.shape[1]):
            norm_recv[phase, pl.ds(at, 1), :] = jnp.zeros((1, LANES), jnp.float32)

    def lines_here():
        pl.semaphore_wait(barrier, expected)
        send_norm(0, 0, HUBS)

    def tell_line():
        if direct:
            for peer, _ in others(n_ta, my_ta):
                pl.semaphore_signal(line_sem, inc=1, device_id={"ta": peer})

    def all_here():
        if direct:
            pl.semaphore_wait(line_sem, n_ta - 1)

    put_norm(0, own_norm)
    norm_first = my_ta > 0

    @pl.when(norm_first)
    def _():
        lines_here()
        tell_line()

    for t, c in chunks[-LATE_SPLITS:]:
        split_sol(t, c)

    def make_signs(lane_maps):
        for copy in small_copies:
            copy.wait()
        signs = []
        for slice_of, column in lane_maps:
            chir = jnp.ones(column.shape, jnp.float32)
            for s in range(srcs):
                for k in range(cols):
                    value = jnp.where(spin_ref[s, k] < 2, 1.0, -1.0)
                    chir = jnp.where(column // spins == s * cols + k, value, chir)
            now = my_ta * slices + slice_of
            sign = chir
            for s in range(srcs):
                value = jnp.where(now < times_ref[s], -chir, chir)
                sign = jnp.where(column // (spins * cols) == s, value, sign)
            signs.append(sign)
        return signs

    def partial(t, c):
        lanes = pl.ds(c * sites, sites)
        both = lax.dot_general(
            sol_split[t, :, lanes], eig_split[t, :, lanes], NT_DIMS,
            preferred_element_type=jnp.float32,
        )
        return both[: parts * columns] + both[parts * columns :]

    def flatten(t, p, tile):
        period = math.lcm(columns, LANES)
        rows_in, rows_out = period // columns, period // LANES
        count = eigs // rows_in
        lane = lax.broadcasted_iota(jnp.int32, (count, LANES), 1)
        tile_buf[t, p] = tile
        taken = [tile_buf[t, p, pl.ds(i, count, stride=rows_in), :] for i in range(rows_in)]
        for o in range(rows_out):
            value, filled = None, 0
            while filled < LANES:
                i, skip = divmod(o * LANES + filled, columns)
                size = min(columns - skip, LANES - filled)
                shift = (filled - skip) % LANES
                part = pltpu.roll(taken[i], shift, 1) if shift else taken[i]
                value = part if value is None else jnp.where(lane < filled, value, part)
                filled += size
            flat_buf[t, p, pl.ds(o, count, stride=rows_out), :] = value

    def store_flat(totals):
        lane = lax.broadcasted_iota(jnp.int32, (1, LANES), 1)
        signs = make_signs([(jnp.full_like(lane, t), lane) for t in range(slices)])
        for t, g in enumerate(totals):
            real, imag = jnp.transpose(g[:columns]), jnp.transpose(g[columns:])
            tiles = real[:eigs] + imag[eigs:], imag[:eigs] - real[eigs:]
            for p in range(parts):
                tile = tiles[p]
                if pad:
                    tile = jnp.concatenate([tile, jnp.zeros((eigs, pad), jnp.float32)], axis=1)
                flatten(t, p, tile * signs[t])
                for d in range(n_sa):
                    send_buf[pl.ds(d * share + t * rows + p * piece, piece), :] = flat_buf[
                        t, p, pl.ds(d * piece, piece), :
                    ]

    def store_packed(totals):
        first, second = totals
        real0, imag0 = first[:columns], first[columns:]
        real1, imag1 = second[:columns], second[columns:]
        front = lax.broadcasted_iota(jnp.int32, (1, LANES), 1) < eigs
        thirds = [slice(i * pad, (i + 1) * pad) for i in range(3)]

        def turn(body, upper, lower):
            tail = jnp.where(front, upper, lower)
            return jnp.transpose(jnp.concatenate([body, tail], axis=0))

        by_real = turn(real0, imag1[thirds[0]], real1[thirds[1]])
        by_imag = turn(imag0, imag1[thirds[1]], -real1[thirds[0]])
        by_both = turn(jnp.where(front, real1, imag1), imag1[thirds[2]], -real1[thirds[2]])
        tiles = (
            by_real[:eigs] + by_imag[eigs:],
            by_imag[:eigs] - by_real[eigs:],
            by_both[:eigs] + by_both[eigs:],
        )
        for i, tile in enumerate(tiles):
            for d in range(n_sa):
                send_buf[pl.ds(d * share + i * piece, piece), :] = tile[
                    d * piece : (d + 1) * piece
                ]

    def send_tiles(begin, end):
        sent = send_buf.reshape(n_sa, share // sub, sub, LANES)
        landed = recv_buf.reshape(n_sa - 1, share // sub, sub, LANES)
        for peer, slot in list(others(n_sa, my_sa))[begin:end]:
            pltpu.make_async_remote_copy(
                src_ref=sent.at[peer],
                dst_ref=landed.at[slot],
                send_sem=out_sems.at[min(begin, 1)],
                recv_sem=in_sem,
                device_id={"sa": peer},
            ).start()

    def first_sent():
        wait_for(recv_buf.at[pl.ds(0, 2 * share)], out_sems.at[0])

    totals = [None] * slices

    def step(c):
        for t in range(slices):
            both = partial(t, c)
            totals[t] = both if c == 0 else totals[t] + both

    wait_for(eig_buf.at[0], eig_sem.at[0])
    for t in range(slices):
        split_eig(t, 0)
    wait_for(eig_buf.at[pl.ds(1, colors - 1)], eig_sem.at[1])
    for c in range(colors):
        if c:
            for t in range(slices):
                split_eig(t, c)
        step(c)
    totals = [
        by_column(t, g[:, : parts * eigs] + g[:, parts * eigs :]) for t, g in enumerate(totals)
    ]
    store_packed(totals) if packed else store_flat(totals)

    @pl.when(jnp.logical_not(norm_first))
    def _():
        lines_here()

    send_tiles(0, 2)

    @pl.when(jnp.logical_not(norm_first))
    def _():
        tell_line()

    all_here()
    send_norm(0, HUBS, None)
    first_sent()
    send_tiles(2, None)

    if len(groups) > 1:
        wait_for(norm_rows(0), norm_in_sems.at[0])
        put_norm(1, jnp.sum(norm_recv[0], axis=0, keepdims=True))
        send_norm(1, 0, None)

    lane = lax.broadcasted_iota(jnp.int32, (SUBLANES, LANES), 1)
    if packed:
        body = lane < columns
        signs = make_signs([
            (jnp.where(body, i // parts, 1), jnp.where(body, lane, lane - columns + i * pad))
            for i in range(3)
        ])
    wait_for(recv_buf, in_sem)
    total = send_buf[pl.ds(my_sa * share, share), :]
    for slot in range(n_sa - 1):
        total = total + recv_buf[pl.ds(slot * share, share), :]

    def join(pieces):
        value = None
        for start, part in pieces:
            value = part if value is None else jnp.where(lane[:1] < start, value, part)
        return value

    def put(t, p, r, value):
        out_ref[p, pl.ds(t, 1), pl.ds(r * LANES, LANES)] = value

    if packed:
        turned = {}
        for i in range(3):
            own = total[i * piece : (i + 1) * piece].reshape(-1, SUBLANES, LANES) * signs[i]
            own = own.reshape(piece, LANES)
            for shift in range(0, LANES, pad):
                turned[i, shift] = pltpu.roll(own, shift, 1) if shift else own
        for r in range(rows_own):
            starts = range(0, LANES, pad)
            from_of = [divmod(r * LANES + start, columns) for start in starts]
            for i in range(3):
                pieces = []
                for start, (row, skip) in zip(starts, from_of):
                    if not start or not skip:
                        pieces.append((start, turned[i, (start - skip) % LANES][row : row + 1]))
                put(i // parts, i % parts, r, join(pieces))
            pieces = [
                (start, turned[skip // pad, (start - columns) % LANES][row : row + 1])
                for start, (row, skip) in zip(starts, from_of)
            ]
            put(1, 1, r, join(pieces))
    else:
        for t in range(slices):
            for p in range(parts):
                for r in range(rows_own):
                    at = t * rows + p * rows_own + r
                    put(t, p, r, total[at : at + 1])
    wait_for(recv_buf.at[pl.ds(2 * share, (n_sa - 3) * share)], out_sems.at[1])
    for phase in range(len(groups)):
        wait_for(norm_rows(phase), norm_out_sems.at[phase])
    final = len(groups) - 1
    wait_for(norm_rows(final), norm_in_sems.at[final])
    rows_by_vreg = norm_recv[final].reshape(-1, SUBLANES, LANES)
    norm_ref[...] = jnp.sum(rows_by_vreg, axis=0)


def hand_over(tiles_ref, norms_ref, out_hbm, norm_hbm, norm_buf, sems):
    tile_copy = pltpu.make_async_copy(tiles_ref, out_hbm, sems.at[0])
    tile_copy.start()
    srcs, cols = norm_buf.shape
    norm = jnp.sum(norms_ref[...], axis=0, keepdims=True)
    for s in range(srcs):
        row = pltpu.roll(norm, LANES - s * cols, 1) if s else norm
        norm_buf[pl.ds(s, 1), :] = row[:, :cols]
    norm_copy = pltpu.make_async_copy(norm_buf, norm_hbm, sems.at[1])
    norm_copy.start()
    tile_copy.wait()
    norm_copy.wait()


def on_device(eigvecs, solutions, source_times, spin_dilution):
    n_ta, n_sa = lax.axis_size("ta"), lax.axis_size("sa")
    parts, slices, eigs, colors, sites = eigvecs.shape
    _, _, srcs, cols, spins, _, _ = solutions.shape
    columns = srcs * cols * spins
    width = eigs * columns // n_sa
    eig_view = jnp.transpose(eigvecs, (0, 1, 3, 2, 4))
    sol_view = jnp.transpose(
        solutions.reshape(parts, slices, srcs * cols, spins, colors, sites // LANES, LANES),
        (0, 1, 2, 4, 5, 3, 6),
    )
    dims = (n_ta, n_sa, parts, slices, eigs, colors, sites, srcs, cols, spins, width)
    blocks = sites // LANES
    inner = colors * sites
    share = slices * parts * (width // LANES)
    len_groups = 1 if n_ta * n_sa <= DIRECT else 2
    most = n_ta * n_sa if n_ta * n_sa <= DIRECT else max(n_ta, n_sa)
    norm_rows = pl.cdiv(most, SUBLANES) * SUBLANES
    f32, bf16 = jnp.float32, jnp.bfloat16
    dma = pltpu.SemaphoreType.DMA
    tiles, norms = pl.pallas_call(
        functools.partial(kernel, dims),
        out_shape=(
            pltpu.VMEM((parts, slices, width), f32),
            pltpu.VMEM((SUBLANES, LANES), f32),
        ),
        in_specs=[
            pl.BlockSpec(memory_space=pltpu.HBM),
            pl.BlockSpec(memory_space=pltpu.HBM),
            pl.BlockSpec(memory_space=pltpu.HBM),
            pl.BlockSpec(memory_space=pltpu.HBM),
        ],
        out_specs=(
            pl.BlockSpec(memory_space=pltpu.VMEM),
            pl.BlockSpec(memory_space=pltpu.VMEM),
        ),
        scratch_shapes=[
            pltpu.VMEM((colors, slices, parts, eigs, sites), f32),
            pltpu.VMEM((slices * colors, parts, columns * (blocks + 1), LANES), f32),
            pltpu.VMEM((slices, 2 * parts * eigs, inner), bf16),
            pltpu.VMEM((slices, 2 * parts * columns, inner), bf16),
            pltpu.VMEM((slices, parts * columns, parts * eigs), f32),
            pltpu.VMEM((slices, parts, eigs, LANES), f32),
            pltpu.VMEM((slices, parts, eigs * columns // LANES, LANES), f32),
            pltpu.VMEM((n_sa * share, LANES), f32),
            pltpu.VMEM(((n_sa - 1) * share, LANES), f32),
            pltpu.VMEM((len_groups, 1, LANES), f32),
            pltpu.VMEM((len_groups, norm_rows, LANES), f32),
            pltpu.SMEM((srcs,), jnp.int32),
            pltpu.SMEM((srcs, cols), jnp.int32),
            dma((2,)),
            dma((2,)),
            dma((slices * colors,)),
            dma((2,)),
            dma,
            dma((len_groups,)),
            dma((len_groups,)),
            pltpu.SemaphoreType.REGULAR,
        ],
        compiler_params=pltpu.CompilerParams(
            collective_id=0, has_side_effects=True, vmem_limit_bytes=66 * 10**6
        ),
    )(eig_view, sol_view, source_times, spin_dilution)
    return pl.pallas_call(
        hand_over,
        out_shape=(
            jax.ShapeDtypeStruct(tiles.shape, f32),
            jax.ShapeDtypeStruct((srcs, cols), f32),
        ),
        in_specs=[pl.BlockSpec(memory_space=pltpu.VMEM)] * 2,
        out_specs=[pl.BlockSpec(memory_space=pltpu.HBM)] * 2,
        scratch_shapes=[pltpu.VMEM((srcs, cols), f32), dma((2,))],
        compiler_params=pltpu.CompilerParams(vmem_limit_bytes=2**20),
    )(tiles, norms)


def solution(mesh):
    return jax.shard_map(
        on_device,
        mesh=mesh,
        in_specs=(
            P(None, "ta", None, None, "sa"),
            P(None, "ta", None, None, None, None, "sa"),
            P(),
            P(),
        ),
        out_specs=(P(None, "ta", "sa"), P()),
        check_vma=False,
    )
```

```python
import functools
import math

import jax
import jax.numpy as jnp
from jax import lax
from jax.experimental import pallas as pl
from jax.experimental.pallas import tpu as pltpu
from jax.sharding import PartitionSpec as P

LANES = 128
SUBLANES = 8
DIRECT = 64
HUBS = 2
LATE_SPLITS = 4
NT_DIMS = (((1,), (1,)), ((), ()))


def split_two(x):
    high = x.astype(jnp.bfloat16)
    low = (x - high.astype(jnp.float32)).astype(jnp.bfloat16)
    return high, low


def others(count, me):
    for k in range(count - 1):
        past = (me <= k).astype(jnp.int32)
        yield k + past, me - 1 + past


def wait_for(ref, sem):
    pltpu.make_async_copy(ref, ref, sem).wait()


def can_pack(parts, slices, eigs, columns, n_sa):
    return (
        parts == slices == 2 and parts * eigs == LANES
        and 4 * columns == 3 * LANES and eigs % (SUBLANES * n_sa) == 0
    )


def kernel(
    dims,
    eig_hbm, sol_hbm, times_hbm, spin_hbm,
    out_ref, norm_ref,
    eig_buf, sol_buf, eig_split, sol_split, g_buf, tile_buf, flat_buf,
    send_buf, recv_buf, norm_send, norm_recv,
    times_ref, spin_ref, small_sem,
    eig_sem, sol_sem, out_sems, in_sem, norm_out_sems, norm_in_sems, line_sem,
):
    n_ta, n_sa, parts, slices, eigs, colors, sites, srcs, cols, spins, width = dims
    columns = srcs * cols * spins
    rows_own = width // LANES
    blocks = sites // LANES
    packed = can_pack(parts, slices, eigs, columns, n_sa)
    pad = LANES - columns
    piece = eigs // n_sa if packed else rows_own
    rows = parts * rows_own
    share = 3 * piece if packed else slices * rows
    sub = math.gcd(share, SUBLANES)
    my_ta, my_sa = lax.axis_index("ta"), lax.axis_index("sa")
    barrier = pltpu.get_barrier_semaphore()

    def flat_device(at):
        return {"ta": lax.div(at, n_sa), "sa": lax.rem(at, n_sa)}

    direct = n_ta * n_sa <= DIRECT
    lines = [
        (n_sa, my_sa, lambda at: {"sa": at}),
        (n_ta, my_ta, lambda at: {"ta": at}),
    ]
    groups = [(n_ta * n_sa, my_ta * n_sa + my_sa, flat_device)] if direct else lines
    chunks = [(t, c) for t in range(slices) for c in range(colors)]

    nodes = srcs * cols
    gap = (blocks + 1) * spins

    def read_sol(t, c):
        at = t * colors + c
        into = sol_buf.at[at].reshape(parts, nodes, blocks + 1, spins, LANES)
        pltpu.make_async_copy(
            sol_hbm.at[:, t, :, c], into.at[:, :, pl.ds(0, blocks)], sol_sem.at[at]
        ).start()

    ahead = len(chunks)
    for t, c in chunks[:ahead]:
        read_sol(t, c)
    for count, me, device in lines:
        for peer, _ in others(count, me):
            pl.semaphore_signal(barrier, inc=1, device_id=device(peer))
    for t, c in chunks[ahead:]:
        read_sol(t, c)
    for c in range(colors):
        for t in range(slices):
            pltpu.make_async_copy(
                eig_hbm.at[:, t, c], eig_buf.at[c, t], eig_sem
            ).start()
    small_copies = [
        pltpu.make_async_copy(times_hbm, times_ref, small_sem.at[0]),
        pltpu.make_async_copy(spin_hbm, spin_ref, small_sem.at[1]),
    ]
    for copy in small_copies:
        copy.start()

    expected = n_sa - 1 + n_ta - 1
    if direct:
        @pl.when((my_ta == 0) & (my_sa < HUBS))
        def _():
            for a in range(1, n_ta):
                for peer, _ in others(n_sa, my_sa):
                    pl.semaphore_signal(barrier, inc=1, device_id={"ta": a, "sa": peer})

        far_hubs = HUBS - (my_sa < HUBS).astype(jnp.int32)
        expected = expected + jnp.where(my_ta > 0, far_hubs, 0)

    def sol_blocks(t, c):
        at = t * colors + c
        for j in range(blocks):
            lanes = pl.ds(c * sites + j * LANES, LANES)
            for p in range(parts):
                x = [
                    sol_buf[at, p, pl.ds(j * spins + spin, nodes, stride=gap), :]
                    for spin in range(spins)
                ]
                yield p, lanes, jnp.concatenate(x, axis=0)

    def split_sol(t, c):
        for p, lanes, x in sol_blocks(t, c):
            high, low = split_two(x)
            sol_split[t, pl.ds(p * columns, columns), lanes] = high
            sol_split[t, pl.ds((parts + p) * columns, columns), lanes] = low

    def by_column(t, g):
        for p in range(parts):
            for spin in range(spins):
                start = (p * spins + spin) * nodes
                g_buf[t, pl.ds(p * columns + spin, nodes, stride=spins), :] = g[
                    start : start + nodes
                ]
        return g_buf[t]

    def split_eig(t, c):
        lanes = pl.ds(c * sites, sites)
        for p in range(parts):
            high, low = split_two(eig_buf[c, t, p])
            eig_split[t, pl.ds(p * eigs, eigs), lanes] = high
            eig_split[t, pl.ds((parts + p) * eigs, eigs), lanes] = low

    squares = jnp.zeros((columns, LANES), jnp.float32)
    for t, c in chunks:
        at = t * colors + c
        into = sol_buf.at[at].reshape(parts, nodes, blocks + 1, spins, LANES)
        wait_for(into.at[:, :, pl.ds(0, blocks)], sol_sem.at[at])
        for _, _, x in sol_blocks(t, c):
            squares = squares + x * x
        if (t, c) not in chunks[-LATE_SPLITS:]:
            split_sol(t, c)

    cells = 1.0 * spins * colors * slices * n_ta * sites * n_sa
    squares = sum(squares[spin * nodes : (spin + 1) * nodes] for spin in range(spins))
    sums = jnp.sum(squares, axis=1, keepdims=True) * (1.0 / cells)
    lane = lax.broadcasted_iota(jnp.int32, (nodes, LANES), 1)
    node = lax.broadcasted_iota(jnp.int32, (nodes, LANES), 0)
    own_norm = jnp.sum(jnp.where(lane == node, sums, 0.0), axis=0, keepdims=True)

    def norm_rows(phase):
        count = groups[phase][0]
        return norm_recv.at[phase].reshape(norm_recv.shape[1], 1, LANES).at[pl.ds(0, count - 1)]

    def send_norm(phase, begin, end):
        count, me, device = groups[phase]
        rows_there = norm_recv.at[phase].reshape(norm_recv.shape[1], 1, LANES)
        for peer, slot in list(others(count, me))[begin:end]:
            pltpu.make_async_remote_copy(
                src_ref=norm_send.at[phase],
                dst_ref=rows_there.at[slot],
                send_sem=norm_out_sems.at[phase],
                recv_sem=norm_in_sems.at[phase],
                device_id=device(peer),
            ).start()

    def put_norm(phase, row):
        count = groups[phase][0]
        norm_send[phase] = row
        norm_recv[phase, pl.ds(count - 1, 1), :] = row
        for at in range(count, norm_recv.shape[1]):
            norm_recv[phase, pl.ds(at, 1), :] = jnp.zeros((1, LANES), jnp.float32)

    def lines_here():
        pl.semaphore_wait(barrier, expected)
        send_norm(0, 0, HUBS)

    def tell_line():
        if direct:
            for peer, _ in others(n_ta, my_ta):
                pl.semaphore_signal(line_sem, inc=1, device_id={"ta": peer})

    def all_here():
        if direct:
            pl.semaphore_wait(line_sem, n_ta - 1)

    put_norm(0, own_norm)
    norm_first = my_ta > 0

    @pl.when(norm_first)
    def _():
        lines_here()
        tell_line()

    for t, c in chunks[-LATE_SPLITS:]:
        split_sol(t, c)

    def make_signs(lane_maps):
        for copy in small_copies:
            copy.wait()
        signs = []
        for slice_of, column in lane_maps:
            chir = jnp.ones(column.shape, jnp.float32)
            for s in range(srcs):
                for k in range(cols):
                    value = jnp.where(spin_ref[s, k] < 2, 1.0, -1.0)
                    chir = jnp.where(column // spins == s * cols + k, value, chir)
            now = my_ta * slices + slice_of
            sign = chir
            for s in range(srcs):
                value = jnp.where(now < times_ref[s], -chir, chir)
                sign = jnp.where(column // (spins * cols) == s, value, sign)
            signs.append(sign)
        return signs

    def partial(t, c):
        lanes = pl.ds(c * sites, sites)
        both = lax.dot_general(
            sol_split[t, :, lanes], eig_split[t, :, lanes], NT_DIMS,
            preferred_element_type=jnp.float32,
        )
        return both[: parts * columns] + both[parts * columns :]

    def flatten(t, p, tile):
        period = math.lcm(columns, LANES)
        rows_in, rows_out = period // columns, period // LANES
        count = eigs // rows_in
        lane = lax.broadcasted_iota(jnp.int32, (count, LANES), 1)
        tile_buf[t, p] = tile
        taken = [tile_buf[t, p, pl.ds(i, count, stride=rows_in), :] for i in range(rows_in)]
        for o in range(rows_out):
            value, filled = None, 0
            while filled < LANES:
                i, skip = divmod(o * LANES + filled, columns)
                size = min(columns - skip, LANES - filled)
                shift = (filled - skip) % LANES
                part = pltpu.roll(taken[i], shift, 1) if shift else taken[i]
                value = part if value is None else jnp.where(lane < filled, value, part)
                filled += size
            flat_buf[t, p, pl.ds(o, count, stride=rows_out), :] = value

    def store_flat(totals):
        lane = lax.broadcasted_iota(jnp.int32, (1, LANES), 1)
        signs = make_signs([(jnp.full_like(lane, t), lane) for t in range(slices)])
        for t, g in enumerate(totals):
            real, imag = jnp.transpose(g[:columns]), jnp.transpose(g[columns:])
            tiles = real[:eigs] + imag[eigs:], imag[:eigs] - real[eigs:]
            for p in range(parts):
                tile = tiles[p]
                if pad:
                    tile = jnp.concatenate([tile, jnp.zeros((eigs, pad), jnp.float32)], axis=1)
                flatten(t, p, tile * signs[t])
                for d in range(n_sa):
                    send_buf[pl.ds(d * share + t * rows + p * piece, piece), :] = flat_buf[
                        t, p, pl.ds(d * piece, piece), :
                    ]

    def store_packed(totals):
        first, second = totals
        real0, imag0 = first[:columns], first[columns:]
        real1, imag1 = second[:columns], second[columns:]
        front = lax.broadcasted_iota(jnp.int32, (1, LANES), 1) < eigs
        thirds = [slice(i * pad, (i + 1) * pad) for i in range(3)]

        def turn(body, upper, lower):
            tail = jnp.where(front, upper, lower)
            return jnp.transpose(jnp.concatenate([body, tail], axis=0))

        by_real = turn(real0, imag1[thirds[0]], real1[thirds[1]])
        by_imag = turn(imag0, imag1[thirds[1]], -real1[thirds[0]])
        by_both = turn(jnp.where(front, real1, imag1), imag1[thirds[2]], -real1[thirds[2]])
        tiles = (
            by_real[:eigs] + by_imag[eigs:],
            by_imag[:eigs] - by_real[eigs:],
            by_both[:eigs] + by_both[eigs:],
        )
        for i, tile in enumerate(tiles):
            for d in range(n_sa):
                send_buf[pl.ds(d * share + i * piece, piece), :] = tile[
                    d * piece : (d + 1) * piece
                ]

    def send_tiles(begin, end):
        sent = send_buf.reshape(n_sa, share // sub, sub, LANES)
        landed = recv_buf.reshape(n_sa - 1, share // sub, sub, LANES)
        for peer, slot in list(others(n_sa, my_sa))[begin:end]:
            pltpu.make_async_remote_copy(
                src_ref=sent.at[peer],
                dst_ref=landed.at[slot],
                send_sem=out_sems.at[min(begin, 1)],
                recv_sem=in_sem,
                device_id={"sa": peer},
            ).start()

    def first_sent():
        wait_for(recv_buf.at[pl.ds(0, 2 * share)], out_sems.at[0])

    totals = [None] * slices

    def step(c):
        for t in range(slices):
            both = partial(t, c)
            totals[t] = both if c == 0 else totals[t] + both

    wait_for(eig_buf, eig_sem)
    for c in range(colors):
        for t in range(slices):
            split_eig(t, c)
        step(c)
    totals = [
        by_column(t, g[:, : parts * eigs] + g[:, parts * eigs :]) for t, g in enumerate(totals)
    ]
    store_packed(totals) if packed else store_flat(totals)

    @pl.when(jnp.logical_not(norm_first))
    def _():
        lines_here()

    send_tiles(0, 2)

    @pl.when(jnp.logical_not(norm_first))
    def _():
        tell_line()

    all_here()
    send_norm(0, HUBS, None)
    first_sent()
    send_tiles(2, None)

    if len(groups) > 1:
        wait_for(norm_rows(0), norm_in_sems.at[0])
        put_norm(1, jnp.sum(norm_recv[0], axis=0, keepdims=True))
        send_norm(1, 0, None)

    lane = lax.broadcasted_iota(jnp.int32, (SUBLANES, LANES), 1)
    if packed:
        body = lane < columns
        signs = make_signs([
            (jnp.where(body, i // parts, 1), jnp.where(body, lane, lane - columns + i * pad))
            for i in range(3)
        ])
    wait_for(recv_buf, in_sem)
    total = send_buf[pl.ds(my_sa * share, share), :]
    for slot in range(n_sa - 1):
        total = total + recv_buf[pl.ds(slot * share, share), :]

    def join(pieces):
        value = None
        for start, part in pieces:
            value = part if value is None else jnp.where(lane[:1] < start, value, part)
        return value

    def put(t, p, r, value):
        out_ref[p, pl.ds(t, 1), pl.ds(r * LANES, LANES)] = value

    if packed:
        turned = {}
        for i in range(3):
            own = total[i * piece : (i + 1) * piece].reshape(-1, SUBLANES, LANES) * signs[i]
            own = own.reshape(piece, LANES)
            for shift in range(0, LANES, pad):
                turned[i, shift] = pltpu.roll(own, shift, 1) if shift else own
        for r in range(rows_own):
            starts = range(0, LANES, pad)
            from_of = [divmod(r * LANES + start, columns) for start in starts]
            for i in range(3):
                pieces = []
                for start, (row, skip) in zip(starts, from_of):
                    if not start or not skip:
                        pieces.append((start, turned[i, (start - skip) % LANES][row : row + 1]))
                put(i // parts, i % parts, r, join(pieces))
            pieces = [
                (start, turned[skip // pad, (start - columns) % LANES][row : row + 1])
                for start, (row, skip) in zip(starts, from_of)
            ]
            put(1, 1, r, join(pieces))
    else:
        for t in range(slices):
            for p in range(parts):
                for r in range(rows_own):
                    at = t * rows + p * rows_own + r
                    put(t, p, r, total[at : at + 1])
    wait_for(recv_buf.at[pl.ds(2 * share, (n_sa - 3) * share)], out_sems.at[1])
    for phase in range(len(groups)):
        wait_for(norm_rows(phase), norm_out_sems.at[phase])
    final = len(groups) - 1
    wait_for(norm_rows(final), norm_in_sems.at[final])
    rows_by_vreg = norm_recv[final].reshape(-1, SUBLANES, LANES)
    norm_ref[...] = jnp.sum(rows_by_vreg, axis=0)


def hand_over(tiles_ref, norms_ref, out_hbm, norm_hbm, norm_buf, sems):
    tile_copy = pltpu.make_async_copy(tiles_ref, out_hbm, sems.at[0])
    tile_copy.start()
    srcs, cols = norm_buf.shape
    norm = jnp.sum(norms_ref[...], axis=0, keepdims=True)
    for s in range(srcs):
        row = pltpu.roll(norm, LANES - s * cols, 1) if s else norm
        norm_buf[pl.ds(s, 1), :] = row[:, :cols]
    norm_copy = pltpu.make_async_copy(norm_buf, norm_hbm, sems.at[1])
    norm_copy.start()
    tile_copy.wait()
    norm_copy.wait()


def on_device(eigvecs, solutions, source_times, spin_dilution):
    n_ta, n_sa = lax.axis_size("ta"), lax.axis_size("sa")
    parts, slices, eigs, colors, sites = eigvecs.shape
    _, _, srcs, cols, spins, _, _ = solutions.shape
    columns = srcs * cols * spins
    width = eigs * columns // n_sa
    eig_view = jnp.transpose(eigvecs, (0, 1, 3, 2, 4))
    sol_view = jnp.transpose(
        solutions.reshape(parts, slices, srcs * cols, spins, colors, sites // LANES, LANES),
        (0, 1, 2, 4, 5, 3, 6),
    )
    dims = (n_ta, n_sa, parts, slices, eigs, colors, sites, srcs, cols, spins, width)
    blocks = sites // LANES
    inner = colors * sites
    share = slices * parts * (width // LANES)
    len_groups = 1 if n_ta * n_sa <= DIRECT else 2
    most = n_ta * n_sa if n_ta * n_sa <= DIRECT else max(n_ta, n_sa)
    norm_rows = pl.cdiv(most, SUBLANES) * SUBLANES
    f32, bf16 = jnp.float32, jnp.bfloat16
    dma = pltpu.SemaphoreType.DMA
    tiles, norms = pl.pallas_call(
        functools.partial(kernel, dims),
        out_shape=(
            pltpu.VMEM((parts, slices, width), f32),
            pltpu.VMEM((SUBLANES, LANES), f32),
        ),
        in_specs=[
            pl.BlockSpec(memory_space=pltpu.HBM),
            pl.BlockSpec(memory_space=pltpu.HBM),
            pl.BlockSpec(memory_space=pltpu.HBM),
            pl.BlockSpec(memory_space=pltpu.HBM),
        ],
        out_specs=(
            pl.BlockSpec(memory_space=pltpu.VMEM),
            pl.BlockSpec(memory_space=pltpu.VMEM),
        ),
        scratch_shapes=[
            pltpu.VMEM((colors, slices, parts, eigs, sites), f32),
            pltpu.VMEM((slices * colors, parts, columns * (blocks + 1), LANES), f32),
            pltpu.VMEM((slices, 2 * parts * eigs, inner), bf16),
            pltpu.VMEM((slices, 2 * parts * columns, inner), bf16),
            pltpu.VMEM((slices, parts * columns, parts * eigs), f32),
            pltpu.VMEM((slices, parts, eigs, LANES), f32),
            pltpu.VMEM((slices, parts, eigs * columns // LANES, LANES), f32),
            pltpu.VMEM((n_sa * share, LANES), f32),
            pltpu.VMEM(((n_sa - 1) * share, LANES), f32),
            pltpu.VMEM((len_groups, 1, LANES), f32),
            pltpu.VMEM((len_groups, norm_rows, LANES), f32),
            pltpu.SMEM((srcs,), jnp.int32),
            pltpu.SMEM((srcs, cols), jnp.int32),
            dma((2,)),
            dma,
            dma((slices * colors,)),
            dma((2,)),
            dma,
            dma((len_groups,)),
            dma((len_groups,)),
            pltpu.SemaphoreType.REGULAR,
        ],
        compiler_params=pltpu.CompilerParams(
            collective_id=0, has_side_effects=True, vmem_limit_bytes=66 * 10**6
        ),
    )(eig_view, sol_view, source_times, spin_dilution)
    return pl.pallas_call(
        hand_over,
        out_shape=(
            jax.ShapeDtypeStruct(tiles.shape, f32),
            jax.ShapeDtypeStruct((srcs, cols), f32),
        ),
        in_specs=[pl.BlockSpec(memory_space=pltpu.VMEM)] * 2,
        out_specs=[pl.BlockSpec(memory_space=pltpu.HBM)] * 2,
        scratch_shapes=[pltpu.VMEM((srcs, cols), f32), dma((2,))],
        compiler_params=pltpu.CompilerParams(vmem_limit_bytes=2**20),
    )(tiles, norms)


def solution(mesh):
    return jax.shard_map(
        on_device,
        mesh=mesh,
        in_specs=(
            P(None, "ta", None, None, "sa"),
            P(None, "ta", None, None, None, None, "sa"),
            P(),
            P(),
        ),
        out_specs=(P(None, "ta", "sa"), P()),
        check_vma=False,
    )
```
